32 devices in a mesh: ep: 8 (over z, x), tp: 4 (over y, core).
Axes of the slice: x: 2, y: 2, z: 4, core: 2. Of those that a mesh axis runs over, the one named last changes fastest.
Arguments:
- tokens: bfloat16 [1024, 3072], P('ep', 'tp'), may hold values from -6 to 6
- expert_ids: int32 [1024, 2], P('ep'), may hold values from 0 to 7, all different within a row
- route_share: float32 [1024], P('ep'), may hold values from 0.5 to 0.95
- w_gate: bfloat16 [65536, 3072], P(('ep', 'tp')), may hold values from -0.109375 to 0.109375
- w_up: bfloat16 [65536, 3072], P(('ep', 'tp')), may hold values from -0.109375 to 0.109375
- w_down: bfloat16 [65536, 3072], P(('ep', 'tp')), may hold values from -0.0625 to 0.0625
- reward_head: float32 [3072], P('tp'), may hold values from -0.109375 to 0.109375
- upstream: bfloat16 [1024, 3072], P('ep', 'tp'), may hold values from -4 to 4
- pair_order: int32 [16], replicated, may hold values from 0 to 15, each once
Outputs:
- layer_out: bfloat16 [1024, 3072], P('ep', 'tp')
- rewards: float32 [16], replicated
- pair_loss: float32 [], replicated
- grad_tokens: bfloat16 [1024, 3072], P('ep', 'tp')
- grad_gate: bfloat16 [65536, 3072], P(('ep', 'tp'))
- grad_up: bfloat16 [65536, 3072], P(('ep', 'tp'))
- grad_down: bfloat16 [65536, 3072], P(('ep', 'tp'))
The draws below stay inside these ranges and needn't reach their ends.
Inputs may be any that keep to these rules, and one draw needn't show every extreme that they name: `expert_ids`: each row names 2 different experts. `pair_order`: each of the 16 sequence indices appears once.
All inputs are finite; a program needn't handle non-finite values.
Results may differ from the reference program's by a relative error of at most 0.014.
Values may be sent and summed in bfloat16 or wider, within the bound.
A program may use at most 128 MiB of HBM per device.

```python
import math
from functools import partial
import jax
import jax.numpy as jnp
from jax import lax

D = 3072
FF = 8192
EXPERTS = 8
TOPK = 2
SEQ_LEN = 64
TOK_DEV = 128
TOKENS = 1024
SEQS = 16
N_EP = 8
N_TP = 4


def shard_levels(own_key, extent, shards, smallest, high):
    factor_of = 1.0
    for axis_at, blocks in shards:
        draws = jax.random.uniform(jax.random.fold_in(jax.random.fold_in(own_key, 6), axis_at), (blocks,), jnp.float32, smallest / len(shards), high / len(shards))
        factor_of = factor_of * jnp.repeat(jnp.exp(draws), extent[axis_at] // blocks).reshape((-1,) + (1,) * (len(extent) - 1 - axis_at))
    return factor_of


def choose_distinct(own_key, rows, count, top, lift):
    sequence = jax.random.permutation(jax.random.fold_in(own_key, 1), count)
    favour = sequence
    for power in range(3):
        favour = favour * favour // count
    favour = favour * lift // count
    lots = jax.random.randint(jax.random.fold_in(own_key, 2), (rows, count), 0, 4096) + favour
    fixed_rows = jax.random.permutation(jax.random.fold_in(own_key, 3), rows)[jnp.arange(count) % rows]
    lots = jnp.where(jnp.arange(rows)[:, None] == fixed_rows[None, :], 1 << 14, lots)
    score = lots * count + jnp.arange(count)
    return lax.top_k(score.astype(jnp.int32), top)[1].astype(jnp.int32)


def centred(rng, extent, deviation, most, split=(), kind=jnp.bfloat16):
    gain = shard_levels(rng, extent, split, -0.22, 0.18) if split else 1.0
    entries = jax.random.normal(rng, extent, jnp.float32) * deviation * gain
    return jnp.minimum(jnp.maximum(entries, -most), most).astype(kind)


def setup_inputs(seed: int = 0) -> dict:
    seeds = jax.random.split(jax.random.key(seed), 10)
    return {
        "tokens": centred(seeds[0], (TOKENS, D), 1.0, 6.0, ((0, 8), (1, 4))),
        "expert_ids": choose_distinct(seeds[1], TOKENS, EXPERTS, TOPK, 2048),
        "route_share": jnp.clip(0.5 + 0.45 * jax.random.uniform(seeds[2], (TOKENS,), jnp.float32) ** shard_levels(seeds[2], (TOKENS,), ((0, 8),), -0.2, 0.2), 0.5, 0.95),
        "w_gate": centred(seeds[3], (EXPERTS * FF, D), D ** -0.5, 0.109375, ((0, 32),)),
        "w_up": centred(seeds[4], (EXPERTS * FF, D), D ** -0.5, 0.109375, ((0, 32),)),
        "w_down": centred(seeds[5], (EXPERTS * FF, D), FF ** -0.5, 0.0625, ((0, 32),)),
        "reward_head": centred(seeds[6], (D,), D ** -0.5, 0.109375, ((0, 4),), jnp.float32),
        "upstream": centred(seeds[7], (TOKENS, D), 0.5, 4.0, ((0, 8), (1, 4))),
        "pair_order": jax.random.permutation(seeds[8], SEQS).astype(jnp.int32),
    }


loss_scale = 256.0
highest = lax.Precision.HIGHEST

def route_tables(expert_ids, route_share, capacity):
    experts_iota = jnp.arange(EXPERTS, dtype=jnp.int32)
    first_hot = (expert_ids[:, 0:1] == experts_iota[None, :]).astype(jnp.int32)
    second_hot = (expert_ids[:, 1:2] == experts_iota[None, :]).astype(jnp.int32)
    first_rank = lax.optimization_barrier(jnp.sum((jnp.cumsum(first_hot, axis=0) - first_hot) * first_hot, axis=1))
    second_before = jnp.cumsum(second_hot, axis=0) - second_hot + lax.optimization_barrier(jnp.sum(first_hot, axis=0))[None, :]
    second_rank = lax.optimization_barrier(jnp.sum(second_before * second_hot, axis=1))
    route_ranks = jnp.stack([first_rank, second_rank], axis=1).astype(jnp.int32)
    route_kept = route_ranks < capacity
    slot_index = jnp.where(route_kept, expert_ids * capacity + route_ranks, -1).astype(jnp.int32)
    shares = jnp.stack([route_share, 1.0 - route_share], axis=1) * route_kept.astype(jnp.float32)
    slot_iota = jnp.arange(EXPERTS * capacity, dtype=jnp.int32)
    matches = (slot_index[:, :, None] == slot_iota[None, None, :]).astype(jnp.float32)
    picker = lax.optimization_barrier(jnp.sum(matches, axis=1))
    mixing = lax.optimization_barrier(jnp.sum(matches * shares[:, :, None], axis=1))
    return (picker, mixing)

def silu_parts(gate_pre):
    sigmoid_value = jax.nn.sigmoid(gate_pre)
    return (gate_pre * sigmoid_value, sigmoid_value * (1.0 + gate_pre * (1.0 - sigmoid_value)))

def block_sum(lefts, rights):
    group_size = FF // (N_EP // EXPERTS * N_TP)
    group_count = FF // group_size
    row_count = lefts[0].shape[0]
    col_count = rights[0].shape[1]
    left_blocks = tuple((matrix.reshape(row_count, group_count, group_size).transpose(1, 0, 2) for matrix in lefts))
    right_blocks = tuple((matrix.reshape(group_count, group_size, col_count) for matrix in rights))

    def accumulate(running, pieces):
        left_set, right_set = pieces
        partial_sum = jnp.dot(left_set[0], right_set[0], preferred_element_type=jnp.float32)
        for position in range(1, len(left_set)):
            partial_sum = partial_sum + jnp.dot(left_set[position], right_set[position], preferred_element_type=jnp.float32)
        rounded = lax.optimization_barrier(partial_sum.astype(jnp.bfloat16))
        return (running + rounded.astype(jnp.float32), None)
    start_value = jnp.zeros((row_count, col_count), jnp.float32)
    return lax.scan(accumulate, start_value, (left_blocks, right_blocks))[0]

def project(rows_in, weight):
    return lax.dot_general(rows_in, weight, (((1,), (1,)), ((), ())), preferred_element_type=jnp.float32)

def expert_forward(operands):
    rows_in, gate_w, up_w, down_w = operands
    gate_pre = project(rows_in, gate_w)
    up_pre = project(rows_in, up_w)
    silu_value, silu_slope = silu_parts(gate_pre)
    hidden = (silu_value * up_pre).astype(jnp.bfloat16)
    return block_sum((hidden,), (down_w,))

def expert_backward(operands):
    rows_in, grads_in, gate_w, up_w, down_w = operands
    gate_pre = project(rows_in, gate_w)
    up_pre = project(rows_in, up_w)
    silu_value, silu_slope = silu_parts(gate_pre)
    hidden = (silu_value * up_pre).astype(jnp.bfloat16)
    hidden_grad = project(grads_in, down_w)
    gate_grad = (hidden_grad * up_pre * silu_slope).astype(jnp.bfloat16)
    up_grad = (hidden_grad * silu_value).astype(jnp.bfloat16)
    contract = (((0,), (0,)), ((), ()))
    grad_down = lax.dot_general(hidden, grads_in, contract, preferred_element_type=jnp.float32).astype(jnp.bfloat16)
    grad_gate = lax.dot_general(gate_grad, rows_in, contract, preferred_element_type=jnp.float32).astype(jnp.bfloat16)
    grad_up = lax.dot_general(up_grad, rows_in, contract, preferred_element_type=jnp.float32).astype(jnp.bfloat16)
    input_sums = block_sum((gate_grad, up_grad), (gate_w, up_w))
    return (grad_gate, grad_up, grad_down, input_sums)

def to_experts(per_source, capacity):
    width = per_source.shape[2]
    arranged = per_source.reshape(N_EP, EXPERTS, capacity, width).transpose(1, 0, 2, 3)
    return arranged.reshape(EXPERTS, N_EP * capacity, width)

def to_sources(per_expert, capacity):
    width = per_expert.shape[2]
    arranged = per_expert.reshape(EXPERTS, N_EP, capacity, width).transpose(1, 0, 2, 3)
    return arranged.reshape(N_EP, EXPERTS * capacity, width)

def reference(tokens, expert_ids, route_share, w_gate, w_up, w_down, reward_head, upstream, pair_order):
    capacity = TOK_DEV * TOPK // EXPERTS
    token_blocks = tokens.reshape(N_EP, TOK_DEV, D).astype(jnp.float32)
    picker, mixing = jax.vmap(partial(route_tables, capacity=capacity))(expert_ids.reshape(N_EP, TOK_DEV, TOPK), route_share.reshape(N_EP, TOK_DEV))
    gathered = jnp.einsum('pts,ptd->psd', picker, token_blocks, precision=highest)
    slot_inputs = to_experts(gathered.astype(jnp.bfloat16), capacity)
    gate_all = w_gate.reshape(EXPERTS, FF, D)
    up_all = w_up.reshape(EXPERTS, FF, D)
    down_all = w_down.reshape(EXPERTS, FF, D)
    expert_out = lax.map(expert_forward, (slot_inputs, gate_all, up_all, down_all))
    mixed_sum = jnp.einsum('pts,psd->ptd', mixing, to_sources(expert_out, capacity), precision=highest)
    layer_out = (token_blocks + mixed_sum).astype(jnp.bfloat16).reshape(TOKENS, D)
    scores = jnp.dot(layer_out.astype(jnp.float32), reward_head, precision=highest)
    rewards = lax.optimization_barrier(jnp.sum(scores.reshape(SEQS, SEQ_LEN), axis=1)) / math.sqrt(SEQ_LEN)
    seq_iota = jnp.arange(SEQS, dtype=jnp.int32)
    chosen_hot = (pair_order[0::2][:, None] == seq_iota[None, :]).astype(jnp.float32)
    rejected_hot = (pair_order[1::2][:, None] == seq_iota[None, :]).astype(jnp.float32)
    margin = jnp.dot(chosen_hot, rewards, precision=highest) - jnp.dot(rejected_hot, rewards, precision=highest)
    pair_loss = jnp.mean(jax.nn.softplus(-margin))
    pair_weight = jax.nn.sigmoid(-margin)
    seq_coef = jnp.dot(pair_weight, rejected_hot - chosen_hot, precision=highest)
    token_coef = jnp.repeat(seq_coef, SEQ_LEN)
    grad_out = (upstream.astype(jnp.float32) + loss_scale * token_coef[:, None] * reward_head[None, :] / math.sqrt(SEQ_LEN)).astype(jnp.bfloat16)
    grad_blocks = grad_out.reshape(N_EP, TOK_DEV, D).astype(jnp.float32)
    slot_grads = to_experts(jnp.einsum('pts,ptd->psd', mixing, grad_blocks, precision=highest).astype(jnp.bfloat16), capacity)
    grad_gate, grad_up, grad_down, input_sums = lax.map(expert_backward, (slot_inputs, slot_grads, gate_all, up_all, down_all))
    returned = jnp.einsum('pts,psd->ptd', picker, to_sources(input_sums, capacity), precision=highest)
    grad_tokens = (grad_blocks + returned).astype(jnp.bfloat16).reshape(TOKENS, D)
    return (layer_out, rewards, pair_loss, grad_tokens, grad_gate.reshape(EXPERTS * FF, D), grad_up.reshape(EXPERTS * FF, D), grad_down.reshape(EXPERTS * FF, D))
```

```python
import math
from functools import partial

import jax
import jax.numpy as jnp
from jax import lax
from jax.experimental import pallas as pl
from jax.experimental.pallas import tpu as pltpu
from jax.sharding import PartitionSpec as P

EXPERTS = 8
SEQ_LEN = 64

loss_scale = 256.0
MESH = pl.DeviceIdType.MESH
NT = (((1,), (1,)), ((), ()))
NN = (((1,), (0,)), ((), ()))
f32 = jnp.float32
bf16 = jnp.bfloat16


def dot(a, b, dims=NN):
    return lax.dot_general(a, b, dims, preferred_element_type=f32)


def remote(src, dst, send_sem, recv_sem, target):
    return pltpu.make_async_remote_copy(
        src_ref=src,
        dst_ref=dst,
        send_sem=send_sem,
        recv_sem=recv_sem,
        device_id=target,
        device_id_type=MESH,
    )


def drain(sent, sem):
    pltpu.make_async_copy(sent, sent, sem).wait()


def layer_kernel(
    n_ep, n_tp, chunks,
    pack_ref, tok_ref, ups_ref, head_ref, pair_ref, wg_ref, wu_ref, wd_ref,
    slots_ref, gslot_ref, hid_ref, gg_ref, ug_ref, layer_ref, gtok_ref, rew_ref, loss_ref,
    wg_v, wu_v, wd_v, tokb, upsb, raw_all, head_all, hp, hc, mixing, picks, meta, meta_t,
    act_a, act_b, uc, rows_a, rows_b, scores, own_row, all_rows, share_row, coef_row, coef_col,
    part_d, pair_d, ybuf_d, sums_d, part_i, pair_i, ybuf_i, sums_i,
    w_sem, local_sem, a2a_send, tok_recv, ups_recv, raw_send, raw_recv, head_send, head_recv,
    tok_tp_send, tok_tp_recv, ups_tp_send, ups_tp_recv, rew_send, rew_recv,
    pair_send, pair_recv_d, pair_recv_i, y_send, y_recv_d, y_recv_i, z_send, z_recv_d, z_recv_i,
):
    q = lax.axis_index("ep")
    t = lax.axis_index("tp")
    count = n_ep * n_tp
    me = q * n_tp + t
    n_y = n_tp // 2
    y = t // 2
    core = t % 2
    partner = y * 2 + 1 - core
    tokens, width = tok_ref.shape
    cap = tokb.shape[1]
    replicas = n_ep // EXPERTS
    depth = slots_ref.shape[2]
    rows = n_ep * cap
    ff = wg_v.shape[0]
    fc = ff // chunks
    per = n_ep // chunks
    lanes = meta.shape[1]
    seq_local = tokens // SEQ_LEN
    seq_scale = loss_scale / math.sqrt(SEQ_LEN)
    expert = q // replicas

    def chunk(c):
        return pl.ds(pl.multiple_of(c * fc, fc), fc)

    def load(c, i, src, dst):
        return pltpu.make_async_copy(src.at[chunk(c)], dst.at[chunk(c)], w_sem.at[i, c])

    for i, (src, dst) in enumerate(((wd_ref, wd_v), (wg_ref, wg_v), (wu_ref, wu_v))):
        for c in range(chunks):
            load(c, i, src, dst).start()

    barrier = pltpu.get_barrier_semaphore()

    def greet(k, carry):
        other = (me + k) % count
        pl.semaphore_signal(
            barrier, inc=1, device_id=(other // n_tp, other % n_tp), device_id_type=MESH
        )
        return carry

    lax.fori_loop(1, count, greet, 0)

    before = (
        lax.broadcasted_iota(jnp.int32, (tokens, tokens), 0)
        < lax.broadcasted_iota(jnp.int32, (tokens, tokens), 1)
    ).astype(f32).astype(bf16)

    def places(first_id, second_id, wanted):
        first = (first_id == wanted).astype(f32)
        second = (second_id == wanted).astype(f32)
        first_rank = dot(first.astype(bf16), before)
        second_rank = dot(second.astype(bf16), before) + jnp.sum(first, axis=1, keepdims=True)
        return first, first_rank, second, second_rank

    experts_iota = lax.broadcasted_iota(jnp.int32, (EXPERTS, tokens), 0).astype(f32)
    pack = pack_ref[...]
    first_id, second_id, share = pack[0:1], pack[1:2], pack[2:3]
    first, first_rank, second, second_rank = places(first_id, second_id, experts_iota)

    def slot_of(hot, rank, ids):
        own_rank = jnp.sum(hot * rank, axis=0, keepdims=True)
        return jnp.where(own_rank < cap, ids * cap + own_rank, -1.0)

    first_slot = slot_of(first, first_rank, first_id)
    second_slot = slot_of(second, second_rank, second_id)
    slot_iota = lax.broadcasted_iota(jnp.int32, (EXPERTS * cap, tokens), 0).astype(f32)
    take = ((slot_iota == first_slot) | (slot_iota == second_slot)).astype(f32).astype(bf16)
    tokb[...] = dot(take, tok_ref[...]).astype(bf16).reshape(EXPERTS, cap, width)
    upsb[...] = dot(take, ups_ref[...]).astype(bf16).reshape(EXPERTS, cap, width)
    pl.semaphore_wait(barrier, count - 1)

    def columns(owner):
        return pl.ds(pl.multiple_of(owner * width, 128), width)

    own = q // replicas
    own_tok = pltpu.make_async_copy(tokb.at[own], slots_ref.at[q, :, columns(t)], local_sem.at[0])
    own_ups = pltpu.make_async_copy(upsb.at[own], gslot_ref.at[q, :, columns(t)], local_sem.at[1])
    own_raw = pltpu.make_async_copy(pack_ref, raw_all.at[q], local_sem.at[2])
    own_head = pltpu.make_async_copy(head_ref, head_all.at[t], local_sem.at[3])

    def spread(buf, out, recv, k):
        to = (q + k) % n_ep
        return remote(
            buf.at[to // replicas], out.at[q, :, columns(t)], a2a_send, recv.at[k], (to, t)
        )

    def arrive(buf, out, recv, k):
        source = (q + n_ep - k) % n_ep
        remote(
            buf.at[0], out.at[source, :, columns(t)], a2a_send, recv.at[k], (source, t)
        ).wait_recv()

    for copy in (own_tok, own_head, own_raw, own_ups):
        copy.start()
    for k in range(1, n_tp):
        remote(
            head_ref, head_all.at[t], head_send, head_recv.at[k], (q, (t + k) % n_tp)
        ).start()

    def send_tok(k, carry):
        spread(tokb, slots_ref, tok_recv, k).start()
        return carry

    lax.fori_loop(1, n_ep, send_tok, 0)

    def send_raw(k, carry):
        to = (q + k) % n_ep
        remote(pack_ref, raw_all.at[q], raw_send, raw_recv.at[k], (to, t)).start()
        return carry

    lax.fori_loop(1, n_ep, send_raw, 0)

    def hand_on(out, sems, k, owner, target, row):
        send, recv = sems
        piece = out.at[(q + n_ep - k) % n_ep, :, columns(owner)]
        return remote(piece, piece, send, recv.at[row, k], (q, target))

    def pass_on(out, sems, k):
        for j in range(1, n_y):
            hand_on(out, sems, k, t, (t + 2 * j) % n_tp, j - 1).start()
        hand_on(out, sems, k, t, partner, n_y - 1).start()

    def forward(out, sems, k):
        for j in range(1, n_y):
            origin = (t + n_tp - 2 * j) % n_tp
            hand_on(out, sems, k, origin, t, j - 1).wait_recv()
            hand_on(out, sems, k, origin, partner, n_y - 1 + j).start()

    def finish(out, sems):
        def one(k, carry):
            hand_on(out, sems, k, partner, t, n_y - 1).wait_recv()
            for j in range(1, n_y):
                origin = (partner + n_tp - 2 * j) % n_tp
                hand_on(out, sems, k, origin, t, n_y - 1 + j).wait_recv()
            return carry

        lax.fori_loop(0, n_ep, one, 0)

    lag = min(2, n_ep)
    tok_sems = (tok_tp_send, tok_tp_recv)
    ups_sems = (ups_tp_send, ups_tp_recv)

    def step_piece(buf, out, recv, sems, own_copy, k):
        @pl.when(k == 0)
        def _():
            own_copy.wait()

        @pl.when(k > 0)
        def _():
            arrive(buf, out, recv, k)

        pass_on(out, sems, k)

        @pl.when(k >= lag)
        def _():
            forward(out, sems, k - lag)

    def last_pieces(out, sems):
        for k in range(n_ep - lag, n_ep):
            forward(out, sems, k)

    own_head.wait()
    tok_f = tok_ref[...].astype(f32)
    head_mine = head_ref[0:1, :]
    own_scores = jnp.sum(tok_f * head_mine, axis=1, keepdims=True)
    token_iota = lax.broadcasted_iota(jnp.int32, (tokens, lanes), 0)
    lane_iota = lax.broadcasted_iota(jnp.int32, (tokens, lanes), 1)
    token_seq = token_iota // SEQ_LEN + q * seq_local
    in_seq = token_seq == lane_iota
    own_row[...] = jnp.broadcast_to(
        jnp.sum(jnp.where(in_seq, own_scores, 0.0), axis=0, keepdims=True), own_row.shape
    )

    back_iota = lax.broadcasted_iota(jnp.int32, (rows, tokens), 0)
    back_slot = ((back_iota // (replicas * cap)) * cap + back_iota % cap).astype(f32)
    is_first = back_slot == first_slot
    is_second = back_slot == second_slot
    mix_t = jnp.where(is_first, share, 0.0) + jnp.where(is_second, 1.0 - share, 0.0)
    mixing[...] = mix_t.T
    picks[...] = (is_first | is_second).astype(f32).T.astype(bf16)

    for k in range(1, n_tp):
        source = (t + n_tp - k) % n_tp
        remote(head_ref, head_all.at[source], head_send, head_recv.at[k], (q, source)).wait_recv()
    part_iota = lax.broadcasted_iota(jnp.int32, (hp.shape[0], width), 0)
    for owner in range(n_tp):
        rest = head_all[owner][0:1, :]
        stacked = jnp.zeros((hp.shape[0], width), f32)
        for i in range(3):
            piece = rest.astype(bf16).astype(f32)
            stacked = jnp.where(part_iota == i, piece, stacked)
            rest = rest - piece
        hp[:, owner * width : (owner + 1) * width] = stacked.astype(bf16)

    def token_phase(c, carry):
        for j in range(per):
            k = c * per + j
            step_piece(tokb, slots_ref, tok_recv, tok_sems, own_tok, k)

            @pl.when(k > 0)
            def _():
                spread(upsb, gslot_ref, ups_recv, k).start()

        load(c, 0, wd_ref, wd_v).wait()
        head_dot = dot(wd_v[chunk(c), :], hp[...], NT)
        hc[chunk(c), :] = jnp.broadcast_to(jnp.sum(head_dot, axis=1, keepdims=True), (fc, 128))
        return carry

    lax.fori_loop(0, chunks, token_phase, 0)
    last_pieces(slots_ref, tok_sems)

    own_raw.wait()

    def raw_wait(k, carry):
        source = (q + n_ep - k) % n_ep
        remote(pack_ref, raw_all.at[source], raw_send, raw_recv.at[k], (source, t)).wait_recv()
        return carry

    lax.fori_loop(1, n_ep, raw_wait, 0)
    cap_iota = lax.broadcasted_iota(jnp.int32, (cap, tokens), 0).astype(f32)
    cap_token = lax.broadcasted_iota(jnp.int32, (cap, tokens), 1) // SEQ_LEN
    cap_lane = lax.broadcasted_iota(jnp.int32, (cap, lanes), 1)
    expert_f = expert.astype(f32)

    def block_meta(b, carry):
        raw = raw_all[b]
        hot = (raw == expert_f).astype(f32)
        rank = dot(hot.astype(bf16), before)
        first_hot, second_hot = hot[0:1], hot[1:2]
        second_of = rank[1:2] + jnp.sum(first_hot, axis=1, keepdims=True)
        first_at = jnp.where((first_hot > 0.0) & (rank[0:1] < cap), rank[0:1], -1.0)
        second_at = jnp.where((second_hot > 0.0) & (second_of < cap), second_of, -1.0)
        share_b = raw[2:3]
        shares = jnp.where(cap_iota == first_at, share_b, 0.0) + jnp.where(
            cap_iota == second_at, 1.0 - share_b, 0.0
        )
        spreaded = jnp.zeros((cap, lanes), f32)
        for s in range(seq_local):
            column = jnp.sum(jnp.where(cap_token == s, shares, 0.0), axis=1, keepdims=True)
            spreaded = jnp.where(cap_lane == b * seq_local + s, column, spreaded)
        meta[pl.ds(pl.multiple_of(b * cap, cap), cap), :] = spreaded
        return carry

    lax.fori_loop(0, n_ep, block_meta, 0)
    meta_t[...] = meta[...].T
    share_row[...] = jnp.broadcast_to(
        jnp.sum(meta_t[...], axis=0, keepdims=True), share_row.shape
    )
    finish(slots_ref, tok_sems)

    scores[...] = jnp.zeros_like(scores)

    def forward_phase(c, carry):
        for j in range(per):
            step_piece(upsb, gslot_ref, ups_recv, ups_sems, own_ups, c * per + j)
        load(c, 1, wg_ref, wg_v).wait()
        load(c, 2, wu_ref, wu_v).wait()
        slot_rows = slots_ref[...].reshape(rows, depth)
        gate = dot(wg_v[chunk(c), :], slot_rows, NT)
        up = dot(wu_v[chunk(c), :], slot_rows, NT)
        sigmoid = jax.nn.sigmoid(gate)
        silu = gate * sigmoid
        act_b[chunk(c), :] = silu
        act_a[chunk(c), :] = up * (sigmoid * (1.0 + gate * (1.0 - sigmoid)))
        hidden = (silu * up).astype(bf16)
        hid_ref[chunk(c), :] = hidden
        hidden_f = hidden.astype(f32)
        rows_a[:, chunk(c)] = hidden_f.T.astype(bf16)
        scores[...] += jnp.sum(hidden_f * hc[chunk(c), 0:1], axis=0, keepdims=True)
        return carry

    lax.fori_loop(0, chunks, forward_phase, 0)
    last_pieces(gslot_ref, ups_sems)

    by_seq = jnp.sum(meta_t[...] * scores[0:1, :], axis=1, keepdims=True)
    mine = own_row[...] + jnp.broadcast_to(by_seq, (lanes, lanes)).T[0:8]
    all_rows[me] = mine

    def send_row(k, carry):
        other = (me + k) % count
        remote(
            all_rows.at[me], all_rows.at[me], rew_send, rew_recv, (other // n_tp, other % n_tp)
        ).start()
        return carry

    lax.fori_loop(1, count, send_row, 0)

    nb = 256 if width % 256 == 0 else 128

    def product(part, target, lefts, weights):
        def tile(n, carry):
            cols = pl.ds(pl.multiple_of(target * width + n * nb, 128), nb)
            total = dot(lefts[0][...], weights[0][:, cols])
            for left, weight in zip(lefts[1:], weights[1:]):
                total = total + dot(left[...], weight[:, cols])
            part[target, :, :, pl.ds(pl.multiple_of(n * nb, 128), nb)] = total.astype(
                bf16
            ).reshape(n_ep, cap, nb)
            return carry

        lax.fori_loop(0, width // nb, tile, 0)

    def to_pair(part, pair, recv, yy):
        return remote(
            part.at[yy * 2 + 1 - core], pair.at[yy], pair_send, recv.at[yy], (q, partner)
        )

    def from_pair(part, pair, recv, yy):
        remote(
            part.at[yy * 2 + core], pair.at[yy], pair_send, recv.at[yy], (q, partner)
        ).wait_recv()

    def over_y(part, pair, ybuf, recv, r, k):
        yy = (y + r) % n_y
        blk = (q + k) % n_ep
        here = part[yy * 2 + core, blk].astype(f32) + pair[yy, blk].astype(f32)
        part[yy * 2 + core, blk] = here.astype(bf16)
        remote(
            part.at[yy * 2 + core, blk], ybuf.at[y, blk], y_send, recv.at[r, k],
            (q, yy * 2 + core),
        ).start()

    def over_z(part, pair, ybuf, sums, y_recv, z_recv, k):
        blk = (q + k) % n_ep
        total = part[t, blk].astype(f32) + pair[y, blk].astype(f32)
        for r in range(1, n_y):
            source = (y + n_y - r) % n_y
            remote(
                part.at[t, blk], ybuf.at[source, blk], y_send, y_recv.at[r, k],
                (q, source * 2 + core),
            ).wait_recv()
            total = total + ybuf[source, blk].astype(f32)

        @pl.when(k == 0)
        def _():
            sums[q] = total.astype(bf16)

        @pl.when(k > 0)
        def _():
            part[t, blk] = total.astype(bf16)
            remote(
                part.at[t, blk], sums.at[q], z_send, z_recv.at[k], (blk, t)
            ).start()

    def all_back(part, sums, z_recv):
        def one(k, carry):
            source = (q + n_ep - k) % n_ep
            remote(
                part.at[t, 0], sums.at[source], z_send, z_recv.at[k], (source, t)
            ).wait_recv()
            return carry

        lax.fori_loop(1, n_ep, one, 0)

    def down_phase(j, carry):
        yy = (y + 1 + j) % n_y
        product(part_d, yy * 2 + 1 - core, (rows_a,), (wd_v,))
        to_pair(part_d, pair_d, pair_recv_d, yy).start()
        product(part_d, yy * 2 + core, (rows_a,), (wd_v,))
        return carry

    lax.fori_loop(0, n_y, down_phase, 0)
    for r in range(n_y):
        from_pair(part_d, pair_d, pair_recv_d, (y + r) % n_y)
    finish(gslot_ref, ups_sems)

    def upstream_phase(c, carry):
        for j in range(per):
            for r in range(1, n_y):
                over_y(part_d, pair_d, ybuf_d, y_recv_d, r, c * per + j)
        uc[chunk(c), :] = dot(wd_v[chunk(c), :], gslot_ref[...].reshape(rows, depth), NT)
        return carry

    lax.fori_loop(0, chunks, upstream_phase, 0)

    rest_rows = all_rows.at[pl.ds(0, count - 1)]
    pltpu.make_async_copy(rest_rows, rest_rows, rew_recv).wait()
    rewards = jnp.sum(all_rows[...], axis=0)[0:1] / math.sqrt(SEQ_LEN)
    rew_ref[...] = jnp.broadcast_to(rewards, rew_ref.shape)
    pairs = pair_ref.shape[0]
    pair_lane = lax.broadcasted_iota(jnp.int32, (pairs, lanes), 1)
    chosen = (pair_lane == pair_ref[:, 0:1]).astype(f32)
    rejected = (pair_lane == pair_ref[:, 1:2]).astype(f32)
    margin = jnp.sum((chosen - rejected) * rewards, axis=1, keepdims=True)
    losses = jnp.maximum(-margin, 0.0) + jnp.log1p(jnp.exp(-jnp.abs(margin)))
    loss_ref[...] = jnp.broadcast_to(
        jnp.sum(losses, axis=0, keepdims=True) / pairs, loss_ref.shape
    )
    pair_weight = jax.nn.sigmoid(-margin)
    seq_coef = jnp.sum(pair_weight * (rejected - chosen), axis=0, keepdims=True)
    slot_coef = seq_scale * jnp.sum(
        jnp.where(meta[...] > 0.0, seq_coef, 0.0), axis=1, keepdims=True
    )
    coef_wide = jnp.broadcast_to(slot_coef, coef_col.shape)
    coef_col[...] = coef_wide
    coef_row[...] = coef_wide.T[0:8]

    def gradient_phase(c, carry):
        for i in range(per):
            k = c * per + i
            over_z(
                part_d, pair_d, ybuf_d, sums_d, y_recv_d, z_recv_d, (k + 1) % n_ep
            )
        hidden_grad = share_row[0:1, :] * (
            uc[chunk(c), :] + coef_row[0:1, :] * hc[chunk(c), 0:1]
        )
        gate_grad = (hidden_grad * act_a[chunk(c), :]).astype(bf16)
        up_grad = (hidden_grad * act_b[chunk(c), :]).astype(bf16)
        gg_ref[chunk(c), :] = gate_grad
        ug_ref[chunk(c), :] = up_grad
        rows_a[:, chunk(c)] = gate_grad.astype(f32).T.astype(bf16)
        rows_b[:, chunk(c)] = up_grad.astype(f32).T.astype(bf16)
        return carry

    lax.fori_loop(0, chunks, gradient_phase, 0)

    def input_phase(j, carry):
        yy = (y + 1 + j) % n_y
        product(part_i, yy * 2 + 1 - core, (rows_a, rows_b), (wg_v, wu_v))
        to_pair(part_i, pair_i, pair_recv_i, yy).start()
        product(part_i, yy * 2 + core, (rows_a, rows_b), (wg_v, wu_v))
        from_pair(part_i, pair_i, pair_recv_i, yy)

        @pl.when(j < n_y - 1)
        def _():
            def one(k, carry_k):
                over_y(part_i, pair_i, ybuf_i, y_recv_i, j + 1, k)
                return carry_k

            lax.fori_loop(0, n_ep, one, 0)

        return carry

    lax.fori_loop(0, n_y, input_phase, 0)

    drain(gslot_ref.at[:, :, pl.ds(0, (n_tp - 1) * width)], ups_tp_send)

    def tail_phase(k, carry):
        row_at = pl.ds(pl.multiple_of(k * cap, cap), cap)
        coef_k = coef_col[row_at, 0:1]
        share_k = jnp.sum(meta[row_at, :], axis=1, keepdims=True)
        for owner in range(n_tp):
            cols = pl.ds(owner * width, width)
            head_k = head_all[owner][0:1, :]
            slot_out = (gslot_ref[k, :, cols].astype(f32) + coef_k * head_k).astype(bf16)
            gslot_ref[k, :, cols] = (share_k * slot_out.astype(f32)).astype(bf16)
        over_z(part_i, pair_i, ybuf_i, sums_i, y_recv_i, z_recv_i, (k + 1) % n_ep)
        return carry

    lax.fori_loop(0, n_ep, tail_phase, 0)

    all_back(part_d, sums_d, z_recv_d)
    rest = mixing[...]
    mixed = tok_ref[...].astype(f32)
    expert_sums = sums_d[...].reshape(rows, width)
    for _ in range(3):
        piece = rest.astype(bf16)
        mixed = mixed + dot(piece, expert_sums)
        rest = rest - piece.astype(f32)
    layer_ref[...] = mixed.astype(bf16)
    token_coef = jnp.sum(jnp.where(in_seq, seq_coef, 0.0), axis=1, keepdims=True)
    grad_out = (ups_ref[...].astype(f32) + seq_scale * token_coef * head_mine).astype(bf16)
    all_back(part_i, sums_i, z_recv_i)
    returned = dot(picks[...], sums_i[...].reshape(rows, width))
    gtok_ref[...] = (grad_out.astype(f32) + returned).astype(bf16)

    drain(sums_d.at[pl.ds(0, n_ep - 1)], a2a_send)
    drain(sums_d.at[pl.ds(0, n_ep - 1)], a2a_send)
    drain(raw_all.at[pl.ds(0, n_ep - 1)], raw_send)
    drain(head_all.at[pl.ds(0, n_tp - 1)], head_send)
    drain(slots_ref.at[:, :, pl.ds(0, (n_tp - 1) * width)], tok_tp_send)
    drain(rest_rows, rew_send)
    for _ in range(2):
        drain(pair_d, pair_send)
        if n_y > 1:
            drain(ybuf_d.at[pl.ds(0, n_y - 1)], y_send)
        drain(sums_d.at[pl.ds(0, n_ep - 1)], z_send)


def run_layer(pack, tokens, upstream, head_rows, pairs, w_gate, w_up, w_down, seq_total, cap):
    n_ep = lax.axis_size("ep")
    n_tp = lax.axis_size("tp")
    n_y = n_tp // 2
    tok_count, width = tokens.shape
    ff, depth = w_gate.shape
    rows = n_ep * cap
    chunks = math.gcd(ff // 256, n_ep)
    lanes = 128 * pl.cdiv(seq_total, 128)
    dma = pltpu.SemaphoreType.DMA
    vmem = pl.BlockSpec(memory_space=pltpu.VMEM)
    hbm = pl.BlockSpec(memory_space=pl.ANY)

    def shape(*dims, kind=bf16):
        return jax.ShapeDtypeStruct(dims, kind)

    def scratch(*dims, kind=bf16):
        return pltpu.VMEM(dims, kind)

    back = [
        scratch(n_tp, n_ep, cap, width), scratch(n_y, n_ep, cap, width),
        scratch(n_y, n_ep, cap, width), scratch(n_ep, cap, width),
    ]
    return pl.pallas_call(
        partial(layer_kernel, n_ep, n_tp, chunks),
        out_shape=(
            shape(n_ep, cap, depth), shape(n_ep, cap, depth),
            shape(ff, rows), shape(ff, rows), shape(ff, rows),
            shape(tok_count, width), shape(tok_count, width),
            shape(8, lanes, kind=f32), shape(8, 128, kind=f32),
        ),
        in_specs=[vmem] * 5 + [hbm] * 3,
        out_specs=[vmem] * 9,
        scratch_shapes=[
            scratch(ff, depth), scratch(ff, depth), scratch(ff, depth),
            scratch(EXPERTS, cap, width), scratch(EXPERTS, cap, width),
            scratch(n_ep, 8, tok_count, kind=f32), scratch(n_tp, 8, width, kind=f32),
            scratch(16, depth), scratch(ff, 128, kind=f32),
            scratch(tok_count, rows, kind=f32), scratch(tok_count, rows),
            scratch(rows, lanes, kind=f32), scratch(lanes, rows, kind=f32),
            scratch(ff, rows, kind=f32), scratch(ff, rows, kind=f32), scratch(ff, rows, kind=f32),
            scratch(rows, ff), scratch(rows, ff),
            scratch(8, rows, kind=f32), scratch(8, lanes, kind=f32),
            scratch(n_ep * n_tp, 8, lanes, kind=f32),
            scratch(8, rows, kind=f32), scratch(8, rows, kind=f32), scratch(rows, 128, kind=f32),
        ] + back + back + [
            dma((3, chunks)), dma((4,)), dma, dma((n_ep,)), dma((n_ep,)), dma, dma((n_ep,)),
            dma, dma((n_tp,)), dma, dma((n_tp - 1, n_ep)), dma, dma((n_tp - 1, n_ep)), dma, dma,
            dma, dma((n_y,)), dma((n_y,)), dma, dma((n_y, n_ep)), dma((n_y, n_ep)),
            dma, dma((n_ep,)), dma((n_ep,)),
        ],
        compiler_params=pltpu.CompilerParams(
            collective_id=0, has_side_effects=True, vmem_limit_bytes=67000000
        ),
        name="run_layer",
    )(pack, tokens, upstream, head_rows, pairs, w_gate, w_up, w_down)


def grads_kernel(hid_ref, gg_ref, ug_ref, slots_ref, gslot_ref, down_ref, gate_ref, up_ref):
    depth = slots_ref.shape[1]
    step = 512 if depth % 512 == 0 else 128

    def tile(n, carry):
        cols = pl.ds(pl.multiple_of(n * step, step), step)
        grads = gslot_ref[:, cols]
        inputs = slots_ref[:, cols]
        down_ref[:, cols] = dot(hid_ref[...], grads).astype(bf16)
        gate_ref[:, cols] = dot(gg_ref[...], inputs).astype(bf16)
        up_ref[:, cols] = dot(ug_ref[...], inputs).astype(bf16)
        return carry

    lax.fori_loop(0, depth // step, tile, 0)


def weight_grads(hid, gg, ug, slots, gslots):
    ff, rows = hid.shape
    depth = slots.shape[1]
    block = 256
    left = pl.BlockSpec((block, rows), lambda i: (i, 0))
    right = pl.BlockSpec((rows, depth), lambda i: (0, 0))
    out = pl.BlockSpec((block, depth), lambda i: (i, 0))
    return pl.pallas_call(
        grads_kernel,
        grid=(ff // block,),
        out_shape=(jax.ShapeDtypeStruct((ff, depth), bf16),) * 3,
        in_specs=[left, left, left, right, right],
        out_specs=[out] * 3,
        compiler_params=pltpu.CompilerParams(vmem_limit_bytes=40000000),
        cost_estimate=pl.CostEstimate(
            flops=6 * ff * rows * depth, bytes_accessed=6 * ff * depth, transcendentals=0
        ),
        name="weight_grads",
    )(hid, gg, ug, slots, gslots)


def per_device(
    tokens, expert_ids, route_share, w_gate, w_up, w_down, reward_head, upstream, pair_order
):
    tok_count, width = tokens.shape
    cap = tok_count * expert_ids.shape[1] // EXPERTS
    seq_total = pair_order.shape[0]
    pack = jnp.concatenate(
        [
            expert_ids.T.astype(f32),
            route_share[None, :],
            jnp.full((5, tok_count), -1.0, f32),
        ],
        axis=0,
    )
    head_rows = jnp.broadcast_to(reward_head[None, :], (8, width))
    pairs = pair_order.reshape(-1, 2)
    slots, gslots, hid, gg, ug, layer_out, grad_tokens, rew, loss = run_layer(
        pack, tokens, upstream, head_rows, pairs, w_gate, w_up, w_down, seq_total, cap
    )
    depth = slots.shape[2]
    grad_down, grad_gate, grad_up = weight_grads(
        hid, gg, ug, slots.reshape(-1, depth), gslots.reshape(-1, depth)
    )
    return (
        layer_out, rew[0, :seq_total], loss[0, 0], grad_tokens, grad_gate, grad_up, grad_down
    )


def solution(mesh):
    in_specs = (
        P("ep", "tp"),
        P("ep", None),
        P("ep"),
        P(("ep", "tp"), None),
        P(("ep", "tp"), None),
        P(("ep", "tp"), None),
        P("tp"),
        P("ep", "tp"),
        P(),
    )
    out_specs = (
        P("ep", "tp"),
        P(),
        P(),
        P("ep", "tp"),
        P(("ep", "tp"), None),
        P(("ep", "tp"), None),
        P(("ep", "tp"), None),
    )
    return jax.shard_map(
        per_device, mesh=mesh, in_specs=in_specs, out_specs=out_specs, check_vma=False
    )
```

```python
import math
from functools import partial

import jax
import jax.numpy as jnp
from jax import lax
from jax.experimental import pallas as pl
from jax.experimental.pallas import tpu as pltpu
from jax.sharding import PartitionSpec as P

EXPERTS = 8
SEQ_LEN = 64

loss_scale = 256.0
MESH = pl.DeviceIdType.MESH
NT = (((1,), (1,)), ((), ()))
NN = (((1,), (0,)), ((), ()))
f32 = jnp.float32
bf16 = jnp.bfloat16


def dot(a, b, dims=NN):
    return lax.dot_general(a, b, dims, preferred_element_type=f32)


def remote(src, dst, send_sem, recv_sem, target):
    return pltpu.make_async_remote_copy(
        src_ref=src,
        dst_ref=dst,
        send_sem=send_sem,
        recv_sem=recv_sem,
        device_id=target,
        device_id_type=MESH,
    )


def drain(sent, sem):
    pltpu.make_async_copy(sent, sent, sem).wait()


def layer_kernel(
    n_ep, n_tp, steps, chunks,
    ids_ref, share_ref, tok_hbm, ups_hbm, head_in, pair_ref, wg_ref, wu_ref, wd_ref,
    slots_hbm, gslot_hbm, hid_hbm, gg_hbm, ug_hbm, layer_hbm, gtok_hbm, rew_hbm, loss_hbm,
    slots_ref, gslot_ref, hid_ref, gg_ref, ug_ref, tok_ref, ups_ref, pack_ref, head_ref,
    layer_ref, gtok_ref, rew_ref, loss_ref,
    wgu_v, wd_v, tokb, upsb, raw_all, head_all, hp, hc, mixing, picks, meta, meta_t,
    act_a, act_b, rows_gu, scores, own_row, all_rows, share_row, coef_row, coef_col,
    part_d, pair_d, ybuf_d, sums_d, part_i, pair_i, ybuf_i, sums_i,
    in_sem, out_sem, big_sem, small_sem, w_sem, local_sem, a2a_send, tok_recv, ups_recv, raw_send, raw_recv, head_send, head_recv,
    tok_tp_send, tok_tp_recv, ups_tp_send, ups_tp_recv, rew_send, rew_recv,
    pair_send, pair_recv_d, pair_recv_i, y_send, y_recv_d, y_recv_i, z_send, z_recv_d, z_recv_i,
):
    q = lax.axis_index("ep")
    t = lax.axis_index("tp")
    count = n_ep * n_tp
    me = q * n_tp + t
    n_y = n_tp // 2
    y = t // 2
    core = t % 2
    partner = y * 2 + 1 - core
    tokens, width = tok_ref.shape
    cap = tokb.shape[1]
    replicas = n_ep // EXPERTS
    depth = slots_ref.shape[2]
    rows = n_ep * cap
    ff = wd_v.shape[0]
    fc = ff // chunks
    per = n_ep // chunks
    per_step = n_ep // steps
    fs = ff // steps
    lanes = meta.shape[1]
    seq_local = tokens // SEQ_LEN
    seq_scale = loss_scale / math.sqrt(SEQ_LEN)
    expert = q // replicas

    def chunk(c):
        return pl.ds(pl.multiple_of(c * fc, fc), fc)

    def step_rows(c):
        return pl.ds(pl.multiple_of(c * fs, fs), fs)

    def load(c, i):
        src = (wd_ref, wg_ref, wu_ref)[i]
        at = step_rows(c) if i == 0 else chunk(c)
        dst = wd_v.at[at] if i == 0 else wgu_v.at[c, pl.ds((i - 1) * fc, fc)]
        return pltpu.make_async_copy(src.at[at], dst, w_sem.at[i, c])

    tok_in = pltpu.make_async_copy(tok_hbm, tok_ref, in_sem.at[0])
    ups_in = pltpu.make_async_copy(ups_hbm, ups_ref, in_sem.at[1])
    tok_in.start()
    ups_in.start()

    def keep(i, src, dst, at):
        return pltpu.make_async_copy(src.at[at], dst.at[at], out_sem.at[i])

    barrier = pltpu.get_barrier_semaphore()

    def greet(k, carry):
        other = (me + k) % count
        pl.semaphore_signal(
            barrier, inc=1, device_id=(other // n_tp, other % n_tp), device_id_type=MESH
        )
        return carry

    lax.fori_loop(1, count, greet, 0)

    before = (
        lax.broadcasted_iota(jnp.int32, (tokens, tokens), 0)
        < lax.broadcasted_iota(jnp.int32, (tokens, tokens), 1)
    ).astype(f32).astype(bf16)

    def places(first_id, second_id, wanted):
        first = (first_id == wanted).astype(f32)
        second = (second_id == wanted).astype(f32)
        first_rank = dot(first.astype(bf16), before)
        second_rank = dot(second.astype(bf16), before) + jnp.sum(first, axis=1, keepdims=True)
        return first, first_rank, second, second_rank

    experts_iota = lax.broadcasted_iota(jnp.int32, (EXPERTS, tokens), 0).astype(f32)
    ids = ids_ref[...].astype(f32)
    first_id, second_id, share = ids[0:1], ids[1:2], share_ref[...]
    pack_iota = lax.broadcasted_iota(jnp.int32, pack_ref.shape, 0)
    pack_ref[...] = jnp.where(
        pack_iota == 0, first_id, jnp.where(pack_iota == 1, second_id, share)
    )
    for i in range(width // 128):
        head_ref[:, i * 128 : (i + 1) * 128] = jnp.broadcast_to(head_in[i : i + 1, :], (8, 128))
    first, first_rank, second, second_rank = places(first_id, second_id, experts_iota)

    def slot_of(hot, rank, ids):
        own_rank = jnp.sum(hot * rank, axis=0, keepdims=True)
        return jnp.where(own_rank < cap, ids * cap + own_rank, -1.0)

    first_slot = slot_of(first, first_rank, first_id)
    second_slot = slot_of(second, second_rank, second_id)
    slot_iota = lax.broadcasted_iota(jnp.int32, (EXPERTS * cap, tokens), 0).astype(f32)
    take = ((slot_iota == first_slot) | (slot_iota == second_slot)).astype(f32).astype(bf16)
    tok_in.wait()
    ups_in.wait()
    for i, many in enumerate((steps, chunks, chunks)):
        for c in range(many):
            load(c, i).start()
    tokb[...] = dot(take, tok_ref[...]).astype(bf16).reshape(EXPERTS, cap, width)
    upsb[...] = dot(take, ups_ref[...]).astype(bf16).reshape(EXPERTS, cap, width)
    pl.semaphore_wait(barrier, count - 1)

    def columns(owner):
        return pl.ds(pl.multiple_of(owner * width, 128), width)

    own = q // replicas
    own_tok = pltpu.make_async_copy(tokb.at[own], slots_ref.at[q, :, columns(t)], local_sem.at[0])
    own_ups = pltpu.make_async_copy(upsb.at[own], gslot_ref.at[q, :, columns(t)], local_sem.at[1])
    own_raw = pltpu.make_async_copy(pack_ref, raw_all.at[q], local_sem.at[2])
    own_head = pltpu.make_async_copy(head_ref, head_all.at[t], local_sem.at[3])

    def spread(buf, out, recv, k):
        to = (q + k) % n_ep
        return remote(
            buf.at[to // replicas], out.at[q, :, columns(t)], a2a_send, recv.at[k], (to, t)
        )

    def arrive(buf, out, recv, k):
        source = (q + n_ep - k) % n_ep
        remote(
            buf.at[0], out.at[source, :, columns(t)], a2a_send, recv.at[k], (source, t)
        ).wait_recv()

    for copy in (own_tok, own_head, own_raw, own_ups):
        copy.start()
    for k in range(1, n_tp):
        remote(
            head_ref, head_all.at[t], head_send, head_recv.at[k], (q, (t + k) % n_tp)
        ).start()

    def send_raw(k, carry):
        to = (q + k) % n_ep
        remote(pack_ref, raw_all.at[q], raw_send, raw_recv.at[k], (to, t)).start()
        return carry

    lax.fori_loop(1, n_ep, send_raw, 0)

    def send_tok(k, carry):
        spread(tokb, slots_ref, tok_recv, k).start()
        return carry

    lax.fori_loop(1, n_ep, send_tok, 0)

    def hand_on(out, sems, k, owner, target, row):
        send, recv = sems
        piece = out.at[(q + n_ep - k) % n_ep, :, columns(owner)]
        return remote(piece, piece, send, recv.at[row, k], (q, target))

    def pass_on(out, sems, k):
        for j in range(1, n_y):
            hand_on(out, sems, k, t, (t + 2 * j) % n_tp, j - 1).start()
        hand_on(out, sems, k, t, partner, n_y - 1).start()

    def forward(out, sems, k):
        for j in range(1, n_y):
            origin = (t + n_tp - 2 * j) % n_tp
            hand_on(out, sems, k, origin, t, j - 1).wait_recv()
            hand_on(out, sems, k, origin, partner, n_y - 1 + j).start()

    def finish(out, sems):
        def one(k, carry):
            hand_on(out, sems, k, partner, t, n_y - 1).wait_recv()
            for j in range(1, n_y):
                origin = (partner + n_tp - 2 * j) % n_tp
                hand_on(out, sems, k, origin, t, n_y - 1 + j).wait_recv()
            return carry

        lax.fori_loop(0, n_ep, one, 0)

    lag = min(2, n_ep)
    tok_sems = (tok_tp_send, tok_tp_recv)
    ups_sems = (ups_tp_send, ups_tp_recv)

    def step_piece(buf, out, recv, sems, k):
        arrive(buf, out, recv, k)
        pass_on(out, sems, k)

        @pl.when(k >= lag)
        def _():
            forward(out, sems, k - lag)

    def last_pieces(out, sems):
        for k in range(n_ep - lag, n_ep):
            forward(out, sems, k)

    own_tok.wait()
    pass_on(slots_ref, tok_sems, 0)

    own_head.wait()
    tok_f = tok_ref[...].astype(f32)
    head_mine = head_ref[0:1, :]
    own_scores = jnp.sum(tok_f * head_mine, axis=1, keepdims=True)
    token_iota = lax.broadcasted_iota(jnp.int32, (tokens, lanes), 0)
    lane_iota = lax.broadcasted_iota(jnp.int32, (tokens, lanes), 1)
    token_seq = token_iota // SEQ_LEN + q * seq_local
    in_seq = token_seq == lane_iota
    own_row[...] = jnp.broadcast_to(
        jnp.sum(jnp.where(in_seq, own_scores, 0.0), axis=0, keepdims=True), own_row.shape
    )

    back_iota = lax.broadcasted_iota(jnp.int32, (rows, tokens), 0)
    back_slot = ((back_iota // (replicas * cap)) * cap + back_iota % cap).astype(f32)
    is_first = back_slot == first_slot
    is_second = back_slot == second_slot
    mix_t = jnp.where(is_first, share, 0.0) + jnp.where(is_second, 1.0 - share, 0.0)
    mixing[...] = mix_t.T
    picks[...] = (is_first | is_second).astype(f32).T.astype(bf16)

    for k in range(1, n_tp):
        source = (t + n_tp - k) % n_tp
        remote(head_ref, head_all.at[source], head_send, head_recv.at[k], (q, source)).wait_recv()
    part_iota = lax.broadcasted_iota(jnp.int32, (hp.shape[0], width), 0)
    for owner in range(n_tp):
        rest = head_all[owner][0:1, :]
        stacked = jnp.zeros((hp.shape[0], width), f32)
        for i in range(3):
            piece = rest.astype(bf16).astype(f32)
            stacked = jnp.where(part_iota == i, piece, stacked)
            rest = rest - piece
        hp[:, owner * width : (owner + 1) * width] = stacked.astype(bf16)

    cap_iota = lax.broadcasted_iota(jnp.int32, (cap, tokens), 0).astype(f32)
    cap_token = lax.broadcasted_iota(jnp.int32, (cap, tokens), 1) // SEQ_LEN
    cap_lane = lax.broadcasted_iota(jnp.int32, (cap, lanes), 1)
    expert_f = expert.astype(f32)

    def block_meta(b):
        raw = raw_all[b]
        hot = (raw == expert_f).astype(f32)
        rank = dot(hot.astype(bf16), before)
        first_hot, second_hot = hot[0:1], hot[1:2]
        second_of = rank[1:2] + jnp.sum(first_hot, axis=1, keepdims=True)
        first_at = jnp.where((first_hot > 0.0) & (rank[0:1] < cap), rank[0:1], -1.0)
        second_at = jnp.where((second_hot > 0.0) & (second_of < cap), second_of, -1.0)
        share_b = raw[2:3]
        shares = jnp.where(cap_iota == first_at, share_b, 0.0) + jnp.where(
            cap_iota == second_at, 1.0 - share_b, 0.0
        )
        spreaded = jnp.zeros((cap, lanes), f32)
        for s in range(seq_local):
            column = jnp.sum(jnp.where(cap_token == s, shares, 0.0), axis=1, keepdims=True)
            spreaded = jnp.where(cap_lane == b * seq_local + s, column, spreaded)
        meta[pl.ds(pl.multiple_of(b * cap, cap), cap), :] = spreaded

    def token_phase(c, carry):
        for j in range(per_step):
            k = c * per_step + j
            source = (q + n_ep - k) % n_ep

            @pl.when(k > 0)
            def _():
                step_piece(tokb, slots_ref, tok_recv, tok_sems, k)
                spread(upsb, gslot_ref, ups_recv, k).start()
                remote(
                    pack_ref, raw_all.at[source], raw_send, raw_recv.at[k], (source, t)
                ).wait_recv()

            block_meta(source)

        load(c, 0).wait()
        head_dot = dot(wd_v[step_rows(c), :], hp[...], NT)
        hc[step_rows(c), :] = jnp.broadcast_to(
            jnp.sum(head_dot, axis=1, keepdims=True), (fs, 128)
        )
        return carry

    own_raw.wait()
    lax.fori_loop(0, steps, token_phase, 0)
    last_pieces(slots_ref, tok_sems)
    meta_t[...] = meta[...].T
    share_row[...] = jnp.broadcast_to(
        jnp.sum(meta_t[...], axis=0, keepdims=True), share_row.shape
    )
    finish(slots_ref, tok_sems)
    slots_out = pltpu.make_async_copy(slots_ref, slots_hbm, big_sem.at[0])
    slots_out.start()

    scores[...] = jnp.zeros_like(scores)

    def gate_up(c):
        load(c, 1).wait()
        load(c, 2).wait()
        slot_rows = slots_ref[...].reshape(rows, depth)
        return dot(wgu_v[c], slot_rows, NT)

    def wide(column):
        return jnp.concatenate([column] * (rows // 128), axis=1)

    def activate(c, products):
        gate, up = products[:fc], products[fc:]
        sigmoid = jax.nn.sigmoid(gate)
        silu = gate * sigmoid
        act_b[chunk(c), :] = silu
        act_a[chunk(c), :] = up * (sigmoid * (1.0 + gate * (1.0 - sigmoid)))
        hidden = (silu * up).astype(bf16)
        hid_ref[chunk(c), :] = hidden
        hidden_f = hidden.astype(f32)
        rows_gu[:, chunk(c)] = hidden_f.T.astype(bf16)
        scores[...] += jnp.sum(
            hidden_f * wide(hc[chunk(c), :]), axis=0, keepdims=True
        )

    def pass_ups(c):
        for j in range(per):
            k = c * per + j

            @pl.when(k > 0)
            def _():
                step_piece(upsb, gslot_ref, ups_recv, ups_sems, k)

    def forward_phase(c, carry):
        pass_ups(c - 1)
        following = gate_up(c)
        activate(c - 1, carry)
        keep(0, hid_ref, hid_hbm, chunk(c - 1)).start()
        return following

    own_ups.wait()
    pass_on(gslot_ref, ups_sems, 0)
    last = lax.fori_loop(1, chunks, forward_phase, gate_up(0))
    activate(chunks - 1, last)
    keep(0, hid_ref, hid_hbm, chunk(chunks - 1)).start()

    by_seq = jnp.sum(meta_t[...] * scores[0:1, :], axis=1, keepdims=True)
    mine = own_row[...] + jnp.broadcast_to(by_seq, (lanes, lanes)).T[0:8]
    all_rows[me] = mine

    def send_row(k, carry):
        other = (me + k) % count
        remote(
            all_rows.at[me], all_rows.at[me], rew_send, rew_recv, (other // n_tp, other % n_tp)
        ).start()
        return carry

    lax.fori_loop(1, count, send_row, 0)

    pass_ups(chunks - 1)

    def within(span):
        return pl.ds(*span)

    def product(part, target, left, weight, span):
        first, size = span
        cols = pl.ds(pl.multiple_of(target * width + first, 128), size)
        total = dot(left[...], weight[:, cols])
        part[target, :, :, within(span)] = total.astype(bf16).reshape(n_ep, cap, size)

    def to_pair(part, pair, recv, span, yy):
        return remote(
            part.at[yy * 2 + 1 - core, :, :, within(span)], pair.at[yy, :, :, within(span)],
            pair_send, recv.at[yy], (q, partner),
        )

    def from_pair(part, pair, recv, span, yy):
        remote(
            part.at[yy * 2 + core, :, :, within(span)], pair.at[yy, :, :, within(span)],
            pair_send, recv.at[yy], (q, partner),
        ).wait_recv()

    def over_y(part, pair, ybuf, recv, span, r, k):
        yy = (y + r) % n_y
        blk = (q + k) % n_ep
        mine_at = (yy * 2 + core, blk, slice(None), within(span))
        here = part[mine_at].astype(f32) + pair[yy, blk, :, within(span)].astype(f32)
        part[mine_at] = here.astype(bf16)
        remote(
            part.at[mine_at], ybuf.at[y, blk, :, within(span)], y_send, recv.at[r - 1, k],
            (q, yy * 2 + core),
        ).start()

    def over_z(part, pair, ybuf, sums, y_recv, z_recv, span, k):
        blk = (q + k) % n_ep
        mine_at = (t, blk, slice(None), within(span))
        total = part[mine_at].astype(f32) + pair[y, blk, :, within(span)].astype(f32)
        for r in range(1, n_y):
            source = (y + n_y - r) % n_y
            remote(
                part.at[mine_at], ybuf.at[source, blk, :, within(span)], y_send,
                y_recv.at[r - 1, k], (q, source * 2 + core),
            ).wait_recv()
            total = total + ybuf[source, blk, :, within(span)].astype(f32)

        @pl.when(k == 0)
        def _():
            sums[q, :, within(span)] = total.astype(bf16)

        @pl.when(k > 0)
        def _():
            part[mine_at] = total.astype(bf16)
            remote(
                part.at[mine_at], sums.at[q, :, within(span)], z_send, z_recv.at[k], (blk, t)
            ).start()

    def all_back(part, sums, z_recv, span):
        def one(k, carry):
            source = (q + n_ep - k) % n_ep
            remote(
                part.at[t, 0, :, within(span)], sums.at[source, :, within(span)], z_send,
                z_recv.at[k], (source, t),
            ).wait_recv()
            return carry

        lax.fori_loop(1, n_ep, one, 0)

    full = (0, width)
    cut = width // 128 * 2 // 3 * 128
    spans = ((0, cut), (cut, width - cut))
    rows_h = rows_gu.at[:, pl.ds(0, ff)]

    def down_phase(j, carry):
        yy = (y + 1 + j) % n_y
        product(part_d, yy * 2 + 1 - core, rows_h, wd_v, full)
        to_pair(part_d, pair_d, pair_recv_d, full, yy).start()
        product(part_d, yy * 2 + core, rows_h, wd_v, full)
        return carry

    lax.fori_loop(0, n_y, down_phase, 0)
    last_pieces(gslot_ref, ups_sems)
    for r in range(n_y):
        from_pair(part_d, pair_d, pair_recv_d, full, (y + r) % n_y)
    finish(gslot_ref, ups_sems)

    rest_rows = all_rows.at[pl.ds(0, count - 1)]
    pltpu.make_async_copy(rest_rows, rest_rows, rew_recv).wait()
    rewards = jnp.sum(all_rows[...], axis=0)[0:1] / math.sqrt(SEQ_LEN)
    seq_total = pair_ref.shape[1]
    rew_ref[...] = rewards[:, :seq_total]
    pairs = seq_total // 2
    pair_lane = lax.broadcasted_iota(jnp.int32, (pairs, lanes), 1).astype(f32)
    order_lane = lax.broadcasted_iota(jnp.int32, (pairs, seq_total), 1)
    order_pair = 2 * lax.broadcasted_iota(jnp.int32, (pairs, seq_total), 0)
    order = pair_ref[...].astype(f32)

    def members(which):
        taken = jnp.where(order_lane == order_pair + which, order, 0.0)
        return (pair_lane == jnp.sum(taken, axis=1, keepdims=True)).astype(f32)

    chosen, rejected = members(0), members(1)
    margin = jnp.sum((chosen - rejected) * rewards, axis=1, keepdims=True)
    losses = jnp.maximum(-margin, 0.0) + jnp.log1p(jnp.exp(-jnp.abs(margin)))
    loss_ref[...] = jnp.sum(losses, axis=0, keepdims=True) / pairs
    pair_weight = jax.nn.sigmoid(-margin)
    seq_coef = jnp.sum(pair_weight * (rejected - chosen), axis=0, keepdims=True)
    slot_coef = seq_scale * jnp.sum(
        jnp.where(meta[...] > 0.0, seq_coef, 0.0), axis=1, keepdims=True
    )
    coef_wide = jnp.broadcast_to(slot_coef, coef_col.shape)
    coef_col[...] = coef_wide
    coef_row[...] = coef_wide.T[0:8]

    pieces = 1
    groups = chunks // pieces
    gc = fc * pieces

    def group(c):
        return pl.ds(pl.multiple_of(c * gc, gc), gc)

    def sums_over_y(c):
        for j in range(per * pieces):
            for r in range(1, n_y):
                over_y(part_d, pair_d, ybuf_d, y_recv_d, full, r, c * per * pieces + j)

    def upstream(c):
        return dot(wd_v[group(c), :], gslot_ref[...].reshape(rows, depth), NT)

    def gradients(c, columns_up):
        hidden_grad = share_row[0:1, :] * (
            columns_up + coef_row[0:1, :] * wide(hc[group(c), :])
        )
        gate_grad = (hidden_grad * act_a[group(c), :]).astype(bf16)
        up_grad = (hidden_grad * act_b[group(c), :]).astype(bf16)
        gg_ref[group(c), :] = gate_grad
        ug_ref[group(c), :] = up_grad
        keep(1, gg_ref, gg_hbm, group(c)).start()
        keep(2, ug_ref, ug_hbm, group(c)).start()
        gate_t = gate_grad.astype(f32).T.astype(bf16)
        up_t = up_grad.astype(f32).T.astype(bf16)
        for i in range(pieces):
            first_at = (c * pieces + i) * 2 * fc
            part_of = slice(i * fc, (i + 1) * fc)
            rows_gu[:, pl.ds(pl.multiple_of(first_at, fc), fc)] = gate_t[:, part_of]
            rows_gu[:, pl.ds(pl.multiple_of(first_at + fc, fc), fc)] = up_t[:, part_of]

    def gradient_phase(c, carry):
        sums_over_y(c)
        following = upstream(c)
        gradients(c - 1, carry)
        return following

    sums_over_y(0)
    last_up = lax.fori_loop(1, groups, gradient_phase, upstream(0))
    gradients(groups - 1, last_up)

    both = wgu_v.reshape(2 * ff, depth)

    share_of = n_ep // n_tp

    def back_some(i):
        for j in range(share_of):
            k = i * share_of + j
            over_z(part_d, pair_d, ybuf_d, sums_d, y_recv_d, z_recv_d, full, (k + 1) % n_ep)

    def return_some(h, i):
        for j in range(share_of):
            k = i * share_of + j
            over_z(
                part_i, pair_i, ybuf_i, sums_i, y_recv_i.at[h], z_recv_i.at[h], spans[h],
                (k + 1) % n_ep,
            )

    def serve(h, i):
        if h == 0:
            back_some(i)
        else:
            return_some(0, i)

    for h in range(2):
        def input_phase(j, carry, h=h):
            yy = (y + 1 + j) % n_y
            product(part_i, yy * 2 + 1 - core, rows_gu, both, spans[h])
            to_pair(part_i, pair_i, pair_recv_i.at[h], spans[h], yy).start()
            serve(h, 2 * j)
            product(part_i, yy * 2 + core, rows_gu, both, spans[h])
            serve(h, 2 * j + 1)
            from_pair(part_i, pair_i, pair_recv_i.at[h], spans[h], yy)

            @pl.when(j < n_y - 1)
            def _():
                def one(k, carry_k):
                    over_y(part_i, pair_i, ybuf_i, y_recv_i.at[h], spans[h], j + 1, k)
                    return carry_k

                lax.fori_loop(0, n_ep, one, 0)

            return carry

        lax.fori_loop(0, n_y, input_phase, 0)

    drain(gslot_ref.at[:, :, pl.ds(0, (n_tp - 1) * width)], ups_tp_send)

    def tail_phase(k, carry):
        row_at = pl.ds(pl.multiple_of(k * cap, cap), cap)
        coef_k = coef_col[row_at, 0:1]
        share_k = jnp.sum(meta[row_at, :], axis=1, keepdims=True)
        for owner in range(n_tp):
            cols = pl.ds(owner * width, width)
            head_k = head_all[owner][0:1, :]
            slot_out = (gslot_ref[k, :, cols].astype(f32) + coef_k * head_k).astype(bf16)
            gslot_ref[k, :, cols] = (share_k * slot_out.astype(f32)).astype(bf16)
        over_z(
            part_i, pair_i, ybuf_i, sums_i, y_recv_i.at[1], z_recv_i.at[1], spans[1],
            (k + 1) % n_ep,
        )
        pltpu.make_async_copy(gslot_ref.at[k], gslot_hbm.at[k], big_sem.at[1]).start()
        return carry

    lax.fori_loop(0, n_ep, tail_phase, 0)

    all_back(part_d, sums_d, z_recv_d, full)
    rest = mixing[...]
    mixed = tok_ref[...].astype(f32)
    expert_sums = sums_d[...].reshape(rows, width)
    for _ in range(3):
        piece = rest.astype(bf16)
        mixed = mixed + dot(piece, expert_sums)
        rest = rest - piece.astype(f32)
    layer_ref[...] = mixed.astype(bf16)
    finals = [
        pltpu.make_async_copy(src, dst, small_sem.at[i])
        for i, (src, dst) in enumerate(
            (
                (layer_ref, layer_hbm), (rew_ref, rew_hbm),
                (loss_ref, loss_hbm), (gtok_ref, gtok_hbm),
            )
        )
    ]
    for copy in finals[:3]:
        copy.start()
    token_coef = jnp.sum(jnp.where(in_seq, seq_coef, 0.0), axis=1, keepdims=True)
    grad_out = (ups_ref[...].astype(f32) + seq_scale * token_coef * head_mine).astype(bf16)
    for h in range(2):
        all_back(part_i, sums_i, z_recv_i.at[h], spans[h])
    returned = dot(picks[...], sums_i[...].reshape(rows, width))
    gtok_ref[...] = (grad_out.astype(f32) + returned).astype(bf16)
    finals[3].start()

    for copy in finals:
        copy.wait()
    slots_out.wait()
    pltpu.make_async_copy(gslot_ref, gslot_hbm, big_sem.at[1]).wait()
    for i, (src, dst) in enumerate(((hid_ref, hid_hbm), (gg_ref, gg_hbm), (ug_ref, ug_hbm))):
        keep(i, src, dst, pl.ds(0, ff)).wait()
    drain(sums_d.at[pl.ds(0, n_ep - 1)], a2a_send)
    drain(sums_d.at[pl.ds(0, n_ep - 1)], a2a_send)
    drain(raw_all.at[pl.ds(0, n_ep - 1)], raw_send)
    drain(head_all.at[pl.ds(0, n_tp - 1)], head_send)
    drain(slots_ref.at[:, :, pl.ds(0, (n_tp - 1) * width)], tok_tp_send)
    drain(rest_rows, rew_send)
    for _ in range(2):
        drain(pair_d, pair_send)
        if n_y > 1:
            drain(ybuf_d.at[pl.ds(0, n_y - 1)], y_send)
        drain(sums_d.at[pl.ds(0, n_ep - 1)], z_send)


def run_layer(
    expert_ids, share, tokens, upstream, head, order, w_gate, w_up, w_down, cap
):
    n_ep = lax.axis_size("ep")
    n_tp = lax.axis_size("tp")
    n_y = n_tp // 2
    tok_count, width = tokens.shape
    ff, depth = w_gate.shape
    rows = n_ep * cap
    steps = math.gcd(ff // 256, n_ep)
    chunks = max(steps // 2, 1)
    fc = ff // chunks
    seq_total = order.shape[1]
    lanes = 128 * pl.cdiv(seq_total, 128)
    dma = pltpu.SemaphoreType.DMA
    vmem = pl.BlockSpec(memory_space=pltpu.VMEM)
    hbm = pl.BlockSpec(memory_space=pl.ANY)

    def shape(*dims, kind=bf16):
        return jax.ShapeDtypeStruct(dims, kind)

    def scratch(*dims, kind=bf16):
        return pltpu.VMEM(dims, kind)

    back = [
        scratch(n_tp, n_ep, cap, width), scratch(n_y, n_ep, cap, width),
        scratch(n_y, n_ep, cap, width), scratch(n_ep, cap, width),
    ]
    return pl.pallas_call(
        partial(layer_kernel, n_ep, n_tp, steps, chunks),
        out_shape=(
            shape(n_ep, cap, depth), shape(n_ep, cap, depth),
            shape(ff, rows), shape(ff, rows), shape(ff, rows),
            shape(tok_count, width), shape(tok_count, width),
            shape(1, seq_total, kind=f32), shape(1, 1, kind=f32),
        ),
        in_specs=[vmem] * 2 + [hbm] * 2 + [vmem] * 2 + [hbm] * 3,
        out_specs=[hbm] * 9,
        scratch_shapes=[
            scratch(n_ep, cap, depth), scratch(n_ep, cap, depth),
            scratch(ff, rows), scratch(ff, rows), scratch(ff, rows),
            scratch(tok_count, width), scratch(tok_count, width),
            scratch(8, tok_count, kind=f32), scratch(8, width, kind=f32),
            scratch(tok_count, width), scratch(tok_count, width),
            scratch(1, seq_total, kind=f32), scratch(1, 1, kind=f32),
            scratch(chunks, 2 * fc, depth), scratch(ff, depth),
            scratch(EXPERTS, cap, width), scratch(EXPERTS, cap, width),
            scratch(n_ep, 8, tok_count, kind=f32), scratch(n_tp, 8, width, kind=f32),
            scratch(16, depth), scratch(ff, 128, kind=f32),
            scratch(tok_count, rows, kind=f32), scratch(tok_count, rows),
            scratch(rows, lanes, kind=f32), scratch(lanes, rows, kind=f32),
            scratch(ff, rows, kind=f32), scratch(ff, rows, kind=f32),
            scratch(rows, 2 * ff),
            scratch(8, rows, kind=f32), scratch(8, lanes, kind=f32),
            scratch(n_ep * n_tp, 8, lanes, kind=f32),
            scratch(8, rows, kind=f32), scratch(8, rows, kind=f32), scratch(rows, 128, kind=f32),
        ] + back + back + [
            dma((2,)), dma((3,)), dma((2,)), dma((4,)),
            dma((3, steps)), dma((4,)), dma, dma((n_ep,)), dma((n_ep,)), dma, dma((n_ep,)),
            dma, dma((n_tp,)), dma, dma((n_tp - 1, n_ep)), dma, dma((n_tp - 1, n_ep)), dma, dma,
            dma, dma((n_y,)), dma((2, n_y)), dma, dma((n_y - 1, n_ep)), dma((2, n_y - 1, n_ep)),
            dma, dma((n_ep,)), dma((2, n_ep)),
        ],
        compiler_params=pltpu.CompilerParams(
            collective_id=0, has_side_effects=True, vmem_limit_bytes=67000000
        ),
        name="run_layer",
    )(expert_ids, share, tokens, upstream, head, order, w_gate, w_up, w_down)


def grads_kernel(
    hid_ref, gg_ref, ug_ref, slots_ref, gslot_ref, layer_in, gtok_in, rew_in, loss_in,
    down_ref, gate_ref, up_ref, layer_ref, gtok_ref, rew_ref, loss_ref,
):
    @pl.when(pl.program_id(0) == 0)
    def _():
        layer_ref[...] = layer_in[...]
        gtok_ref[...] = gtok_in[...]
        rew_ref[...] = rew_in[...]
        loss_ref[...] = loss_in[...]

    inputs = slots_ref[...]
    down_ref[...] = dot(hid_ref[...], gslot_ref[...]).astype(bf16)
    gate_ref[...] = dot(gg_ref[...], inputs).astype(bf16)
    up_ref[...] = dot(ug_ref[...], inputs).astype(bf16)


def weight_grads(hid, gg, ug, slots, gslots, *small):
    ff, rows = hid.shape
    depth = slots.shape[1]
    block = 512 if depth % 512 == 0 else 128

    def whole(array):
        return pl.BlockSpec(array.shape, lambda i: (0, 0))

    left = pl.BlockSpec((ff, rows), lambda i: (0, 0))
    right = pl.BlockSpec((rows, block), lambda i: (0, i))
    out = pl.BlockSpec((ff, block), lambda i: (0, i))
    return pl.pallas_call(
        grads_kernel,
        grid=(depth // block,),
        out_shape=(jax.ShapeDtypeStruct((ff, depth), bf16),) * 3
        + tuple(jax.ShapeDtypeStruct(array.shape, array.dtype) for array in small),
        in_specs=[left, left, left, right, right] + [whole(array) for array in small],
        out_specs=[out] * 3 + [whole(array) for array in small],
        compiler_params=pltpu.CompilerParams(vmem_limit_bytes=67000000),
        cost_estimate=pl.CostEstimate(
            flops=6 * ff * rows * depth, bytes_accessed=6 * ff * depth, transcendentals=0
        ),
        name="weight_grads",
    )(hid, gg, ug, slots, gslots, *small)


def per_device(
    tokens, expert_ids, route_share, w_gate, w_up, w_down, reward_head, upstream, pair_order
):
    tok_count = tokens.shape[0]
    cap = tok_count * expert_ids.shape[1] // EXPERTS
    slots, gslots, hid, gg, ug, *small = run_layer(
        expert_ids.T, route_share.reshape(1, -1), tokens, upstream, reward_head.reshape(-1, 128),
        pair_order.reshape(1, -1), w_gate, w_up, w_down, cap,
    )
    depth = slots.shape[2]
    grad_down, grad_gate, grad_up, layer_out, grad_tokens, rew, loss = weight_grads(
        hid, gg, ug, slots.reshape(-1, depth), gslots.reshape(-1, depth), *small
    )
    return (
        layer_out, rew.reshape(-1), loss.reshape(()), grad_tokens, grad_gate, grad_up, grad_down
    )


def solution(mesh):
    in_specs = (
        P("ep", "tp"),
        P("ep", None),
        P("ep"),
        P(("ep", "tp"), None),
        P(("ep", "tp"), None),
        P(("ep", "tp"), None),
        P("tp"),
        P("ep", "tp"),
        P(),
    )
    out_specs = (
        P("ep", "tp"),
        P(),
        P(),
        P("ep", "tp"),
        P(("ep", "tp"), None),
        P(("ep", "tp"), None),
        P(("ep", "tp"), None),
    )
    return jax.shard_map(
        per_device, mesh=mesh, in_specs=in_specs, out_specs=out_specs, check_vma=False
    )
```

```python
import math
from functools import partial

import jax
import jax.numpy as jnp
from jax import lax
from jax.experimental import pallas as pl
from jax.experimental.pallas import tpu as pltpu
from jax.sharding import PartitionSpec as P

EXPERTS = 8
SEQ_LEN = 64

loss_scale = 256.0
MESH = pl.DeviceIdType.MESH
NT = (((1,), (1,)), ((), ()))
NN = (((1,), (0,)), ((), ()))
f32 = jnp.float32
bf16 = jnp.bfloat16


def dot(a, b, dims=NN):
    return lax.dot_general(a, b, dims, preferred_element_type=f32)


def remote(src, dst, send_sem, recv_sem, target):
    return pltpu.make_async_remote_copy(
        src_ref=src,
        dst_ref=dst,
        send_sem=send_sem,
        recv_sem=recv_sem,
        device_id=target,
        device_id_type=MESH,
    )


def drain(sent, sem):
    pltpu.make_async_copy(sent, sent, sem).wait()


def layer_kernel(
    n_ep, n_tp, steps, chunks,
    ids_ref, share_ref, tok_hbm, ups_hbm, head_in, pair_ref, wg_ref, wu_ref, wd_ref,
    slots_hbm, gslot_hbm, hid_hbm, gg_hbm, ug_hbm, layer_hbm, gtok_hbm, rew_hbm, loss_hbm,
    slots_ref, gslot_ref, hid_ref, gg_ref, ug_ref, tok_ref, ups_ref, pack_ref, head_ref,
    layer_ref, gtok_ref, rew_ref, loss_ref,
    wgu_v, wd_v, tokb, upsb, raw_all, head_all, hp, hc, mixing, picks, meta, meta_t,
    act_a, act_b, rows_gu, scores, own_row, all_rows, share_row, coef_row, coef_col,
    part_d, pair_d, ybuf_d, sums_d, part_i, pair_i, ybuf_i, sums_i,
    in_sem, out_sem, big_sem, small_sem, w_sem, local_sem, a2a_send, tok_recv, ups_recv, raw_send, raw_recv, head_send, head_recv,
    tok_tp_send, tok_tp_recv, ups_tp_send, ups_tp_recv, rew_send, rew_recv,
    pair_send, pair_recv_d, pair_recv_i, y_send, y_recv_d, y_recv_i, z_send, z_recv_d, z_recv_i,
):
    q = lax.axis_index("ep")
    t = lax.axis_index("tp")
    count = n_ep * n_tp
    me = q * n_tp + t
    n_y = n_tp // 2
    y = t // 2
    core = t % 2
    partner = y * 2 + 1 - core
    tokens, width = tok_ref.shape
    cap = tokb.shape[1]
    replicas = n_ep // EXPERTS
    depth = slots_ref.shape[2]
    rows = n_ep * cap
    ff = wd_v.shape[0]
    fc = ff // chunks
    per = n_ep // chunks
    per_step = n_ep // steps
    fs = ff // steps
    lanes = meta.shape[1]
    seq_local = tokens // SEQ_LEN
    seq_scale = loss_scale / math.sqrt(SEQ_LEN)
    expert = q // replicas

    def chunk(c):
        return pl.ds(pl.multiple_of(c * fc, fc), fc)

    def step_rows(c):
        return pl.ds(pl.multiple_of(c * fs, fs), fs)

    def load(c, i):
        src = (wd_ref, wg_ref, wu_ref)[i]
        at = step_rows(c) if i == 0 else chunk(c)
        dst = wd_v.at[at] if i == 0 else wgu_v.at[c, pl.ds((i - 1) * fc, fc)]
        return pltpu.make_async_copy(src.at[at], dst, w_sem.at[i, c])

    tok_in = pltpu.make_async_copy(tok_hbm, tok_ref, in_sem.at[0])
    ups_in = pltpu.make_async_copy(ups_hbm, ups_ref, in_sem.at[1])
    tok_in.start()
    ups_in.start()

    def keep(i, src, dst, at):
        return pltpu.make_async_copy(src.at[at], dst.at[at], out_sem.at[i])

    barrier = pltpu.get_barrier_semaphore()

    def greet(k, carry):
        other = (me + k) % count
        pl.semaphore_signal(
            barrier, inc=1, device_id=(other // n_tp, other % n_tp), device_id_type=MESH
        )
        return carry

    lax.fori_loop(1, count, greet, 0)

    before = (
        lax.broadcasted_iota(jnp.int32, (tokens, tokens), 0)
        < lax.broadcasted_iota(jnp.int32, (tokens, tokens), 1)
    ).astype(f32).astype(bf16)

    def places(first_id, second_id, wanted):
        first = (first_id == wanted).astype(f32)
        second = (second_id == wanted).astype(f32)
        first_rank = dot(first.astype(bf16), before)
        second_rank = dot(second.astype(bf16), before) + jnp.sum(first, axis=1, keepdims=True)
        return first, first_rank, second, second_rank

    experts_iota = lax.broadcasted_iota(jnp.int32, (EXPERTS, tokens), 0).astype(f32)
    ids = ids_ref[...].astype(f32)
    first_id, second_id, share = ids[0:1], ids[1:2], share_ref[...]
    pack_iota = lax.broadcasted_iota(jnp.int32, pack_ref.shape, 0)
    pack_ref[...] = jnp.where(
        pack_iota == 0, first_id, jnp.where(pack_iota == 1, second_id, share)
    )
    for i in range(width // 128):
        head_ref[:, i * 128 : (i + 1) * 128] = jnp.broadcast_to(head_in[i : i + 1, :], (8, 128))
    first, first_rank, second, second_rank = places(first_id, second_id, experts_iota)

    def slot_of(hot, rank, ids):
        own_rank = jnp.sum(hot * rank, axis=0, keepdims=True)
        return jnp.where(own_rank < cap, ids * cap + own_rank, -1.0)

    first_slot = slot_of(first, first_rank, first_id)
    second_slot = slot_of(second, second_rank, second_id)
    slot_iota = lax.broadcasted_iota(jnp.int32, (EXPERTS * cap, tokens), 0).astype(f32)
    take = ((slot_iota == first_slot) | (slot_iota == second_slot)).astype(f32).astype(bf16)
    tok_in.wait()
    ups_in.wait()
    for i, many in enumerate((steps, chunks, chunks)):
        for c in range(many):
            load(c, i).start()
    tokb[...] = dot(take, tok_ref[...]).astype(bf16).reshape(EXPERTS, cap, width)
    upsb[...] = dot(take, ups_ref[...]).astype(bf16).reshape(EXPERTS, cap, width)
    pl.semaphore_wait(barrier, count - 1)

    def columns(owner):
        return pl.ds(pl.multiple_of(owner * width, 128), width)

    own = q // replicas
    own_tok = pltpu.make_async_copy(tokb.at[own], slots_ref.at[q, :, columns(t)], local_sem.at[0])
    own_ups = pltpu.make_async_copy(upsb.at[own], gslot_ref.at[q, :, columns(t)], local_sem.at[1])
    own_raw = pltpu.make_async_copy(pack_ref, raw_all.at[q], local_sem.at[2])
    own_head = pltpu.make_async_copy(head_ref, head_all.at[t], local_sem.at[3])

    def spread(buf, out, recv, k):
        to = (q + k) % n_ep
        return remote(
            buf.at[to // replicas], out.at[q, :, columns(t)], a2a_send, recv.at[k], (to, t)
        )

    def arrive(buf, out, recv, k):
        source = (q + n_ep - k) % n_ep
        remote(
            buf.at[0], out.at[source, :, columns(t)], a2a_send, recv.at[k], (source, t)
        ).wait_recv()

    for copy in (own_tok, own_head, own_raw, own_ups):
        copy.start()
    for k in range(1, n_tp):
        remote(
            head_ref, head_all.at[t], head_send, head_recv.at[k], (q, (t + k) % n_tp)
        ).start()

    def send_raw(k, carry):
        to = (q + k) % n_ep
        remote(pack_ref, raw_all.at[q], raw_send, raw_recv.at[k], (to, t)).start()
        return carry

    lax.fori_loop(1, n_ep, send_raw, 0)

    def send_tok(k, carry):
        spread(tokb, slots_ref, tok_recv, k).start()
        return carry

    lax.fori_loop(1, n_ep, send_tok, 0)

    def hand_on(out, sems, k, owner, target, row):
        send, recv = sems
        piece = out.at[(q + n_ep - k) % n_ep, :, columns(owner)]
        return remote(piece, piece, send, recv.at[row, k], (q, target))

    def pass_on(out, sems, k):
        for j in range(1, n_y):
            hand_on(out, sems, k, t, (t + 2 * j) % n_tp, j - 1).start()
        hand_on(out, sems, k, t, partner, n_y - 1).start()

    def forward(out, sems, k):
        for j in range(1, n_y):
            origin = (t + n_tp - 2 * j) % n_tp
            hand_on(out, sems, k, origin, t, j - 1).wait_recv()
            hand_on(out, sems, k, origin, partner, n_y - 1 + j).start()

    def finish(out, sems):
        def one(k, carry):
            hand_on(out, sems, k, partner, t, n_y - 1).wait_recv()
            for j in range(1, n_y):
                origin = (partner + n_tp - 2 * j) % n_tp
                hand_on(out, sems, k, origin, t, n_y - 1 + j).wait_recv()
            return carry

        lax.fori_loop(0, n_ep, one, 0)

    lag = min(2, n_ep)
    tok_sems = (tok_tp_send, tok_tp_recv)
    ups_sems = (ups_tp_send, ups_tp_recv)

    def step_piece(buf, out, recv, sems, k):
        arrive(buf, out, recv, k)
        pass_on(out, sems, k)

        @pl.when(k >= lag)
        def _():
            forward(out, sems, k - lag)

    def last_pieces(out, sems):
        for k in range(n_ep - lag, n_ep):
            forward(out, sems, k)

    own_tok.wait()
    pass_on(slots_ref, tok_sems, 0)

    own_head.wait()
    tok_f = tok_ref[...].astype(f32)
    head_mine = head_ref[0:1, :]
    own_scores = jnp.sum(tok_f * head_mine, axis=1, keepdims=True)
    token_iota = lax.broadcasted_iota(jnp.int32, (tokens, lanes), 0)
    lane_iota = lax.broadcasted_iota(jnp.int32, (tokens, lanes), 1)
    token_seq = token_iota // SEQ_LEN + q * seq_local
    in_seq = token_seq == lane_iota
    own_row[...] = jnp.broadcast_to(
        jnp.sum(jnp.where(in_seq, own_scores, 0.0), axis=0, keepdims=True), own_row.shape
    )

    back_iota = lax.broadcasted_iota(jnp.int32, (rows, tokens), 0)
    back_slot = ((back_iota // (replicas * cap)) * cap + back_iota % cap).astype(f32)
    is_first = back_slot == first_slot
    is_second = back_slot == second_slot
    mix_t = jnp.where(is_first, share, 0.0) + jnp.where(is_second, 1.0 - share, 0.0)
    mixing[...] = mix_t.T
    picks[...] = (is_first | is_second).astype(f32).T.astype(bf16)

    for k in range(1, n_tp):
        source = (t + n_tp - k) % n_tp
        remote(head_ref, head_all.at[source], head_send, head_recv.at[k], (q, source)).wait_recv()
    part_iota = lax.broadcasted_iota(jnp.int32, (hp.shape[0], width), 0)
    for owner in range(n_tp):
        rest = head_all[owner][0:1, :]
        stacked = jnp.zeros((hp.shape[0], width), f32)
        for i in range(3):
            piece = rest.astype(bf16).astype(f32)
            stacked = jnp.where(part_iota == i, piece, stacked)
            rest = rest - piece
        hp[:, owner * width : (owner + 1) * width] = stacked.astype(bf16)

    cap_iota = lax.broadcasted_iota(jnp.int32, (cap, tokens), 0).astype(f32)
    cap_token = lax.broadcasted_iota(jnp.int32, (cap, tokens), 1) // SEQ_LEN
    cap_lane = lax.broadcasted_iota(jnp.int32, (cap, lanes), 1)
    expert_f = expert.astype(f32)

    def block_meta(b):
        raw = raw_all[b]
        hot = (raw == expert_f).astype(f32)
        rank = dot(hot.astype(bf16), before)
        first_hot, second_hot = hot[0:1], hot[1:2]
        second_of = rank[1:2] + jnp.sum(first_hot, axis=1, keepdims=True)
        first_at = jnp.where((first_hot > 0.0) & (rank[0:1] < cap), rank[0:1], -1.0)
        second_at = jnp.where((second_hot > 0.0) & (second_of < cap), second_of, -1.0)
        share_b = raw[2:3]
        shares = jnp.where(cap_iota == first_at, share_b, 0.0) + jnp.where(
            cap_iota == second_at, 1.0 - share_b, 0.0
        )
        spreaded = jnp.zeros((cap, lanes), f32)
        for s in range(seq_local):
            column = jnp.sum(jnp.where(cap_token == s, shares, 0.0), axis=1, keepdims=True)
            spreaded = jnp.where(cap_lane == b * seq_local + s, column, spreaded)
        meta[pl.ds(pl.multiple_of(b * cap, cap), cap), :] = spreaded

    def token_phase(c, carry):
        for j in range(per_step):
            k = c * per_step + j
            source = (q + n_ep - k) % n_ep

            @pl.when(k > 0)
            def _():
                step_piece(tokb, slots_ref, tok_recv, tok_sems, k)
                spread(upsb, gslot_ref, ups_recv, k).start()
                remote(
                    pack_ref, raw_all.at[source], raw_send, raw_recv.at[k], (source, t)
                ).wait_recv()

            block_meta(source)

        load(c, 0).wait()
        head_dot = dot(wd_v[step_rows(c), :], hp[...], NT)
        hc[step_rows(c), :] = jnp.broadcast_to(
            jnp.sum(head_dot, axis=1, keepdims=True), (fs, 128)
        )
        return carry

    own_raw.wait()
    lax.fori_loop(0, steps, token_phase, 0)
    last_pieces(slots_ref, tok_sems)
    meta_t[...] = meta[...].T
    share_row[...] = jnp.broadcast_to(
        jnp.sum(meta_t[...], axis=0, keepdims=True), share_row.shape
    )
    finish(slots_ref, tok_sems)
    slots_out = pltpu.make_async_copy(slots_ref, slots_hbm, big_sem.at[0])
    slots_out.start()

    scores[...] = jnp.zeros_like(scores)

    def gate_up(c):
        load(c, 1).wait()
        load(c, 2).wait()
        slot_rows = slots_ref[...].reshape(rows, depth)
        return dot(wgu_v[c], slot_rows, NT)

    def wide(column):
        return jnp.concatenate([column] * (rows // 128), axis=1)

    def activate(c, products):
        gate, up = products[:fc], products[fc:]
        sigmoid = jax.nn.sigmoid(gate)
        silu = gate * sigmoid
        act_b[chunk(c), :] = silu
        act_a[chunk(c), :] = up * (sigmoid * (1.0 + gate * (1.0 - sigmoid)))
        hidden = (silu * up).astype(bf16)
        hid_ref[chunk(c), :] = hidden
        hidden_f = hidden.astype(f32)
        rows_gu[:, chunk(c)] = hidden_f.T.astype(bf16)
        scores[...] += jnp.sum(
            hidden_f * wide(hc[chunk(c), :]), axis=0, keepdims=True
        )

    def pass_ups(c):
        for j in range(per):
            k = c * per + j

            @pl.when(k > 0)
            def _():
                step_piece(upsb, gslot_ref, ups_recv, ups_sems, k)

    def forward_phase(c, carry):
        pass_ups(c - 1)
        following = gate_up(c)
        activate(c - 1, carry)
        keep(0, hid_ref, hid_hbm, chunk(c - 1)).start()
        return following

    own_ups.wait()
    pass_on(gslot_ref, ups_sems, 0)
    last = lax.fori_loop(1, chunks, forward_phase, gate_up(0))
    activate(chunks - 1, last)
    keep(0, hid_ref, hid_hbm, chunk(chunks - 1)).start()

    by_seq = jnp.sum(meta_t[...] * scores[0:1, :], axis=1, keepdims=True)
    mine = own_row[...] + jnp.broadcast_to(by_seq, (lanes, lanes)).T[0:8]
    all_rows[me] = mine

    def send_row(k, carry):
        other = (me + k) % count
        remote(
            all_rows.at[me], all_rows.at[me], rew_send, rew_recv, (other // n_tp, other % n_tp)
        ).start()
        return carry

    lax.fori_loop(1, count, send_row, 0)

    pass_ups(chunks - 1)

    def within(span):
        return pl.ds(*span)

    def product(part, target, left, weight, span):
        first, size = span
        cols = pl.ds(pl.multiple_of(target * width + first, 128), size)
        total = dot(left[...], weight[:, cols])
        part[target, :, :, within(span)] = total.astype(bf16).reshape(n_ep, cap, size)

    def to_pair(part, pair, recv, span, yy):
        return remote(
            part.at[yy * 2 + 1 - core, :, :, within(span)], pair.at[yy, :, :, within(span)],
            pair_send, recv.at[yy], (q, partner),
        )

    def from_pair(part, pair, recv, span, yy):
        remote(
            part.at[yy * 2 + core, :, :, within(span)], pair.at[yy, :, :, within(span)],
            pair_send, recv.at[yy], (q, partner),
        ).wait_recv()

    def over_y(part, pair, ybuf, recv, span, r, k):
        yy = (y + r) % n_y
        blk = (q + k) % n_ep
        mine_at = (yy * 2 + core, blk, slice(None), within(span))
        here = part[mine_at].astype(f32) + pair[yy, blk, :, within(span)].astype(f32)
        part[mine_at] = here.astype(bf16)
        remote(
            part.at[mine_at], ybuf.at[y, blk, :, within(span)], y_send, recv.at[r - 1, k],
            (q, yy * 2 + core),
        ).start()

    def over_z(part, pair, ybuf, sums, y_recv, z_recv, span, k):
        blk = (q + k) % n_ep
        mine_at = (t, blk, slice(None), within(span))
        total = part[mine_at].astype(f32) + pair[y, blk, :, within(span)].astype(f32)
        for r in range(1, n_y):
            source = (y + n_y - r) % n_y
            remote(
                part.at[mine_at], ybuf.at[source, blk, :, within(span)], y_send,
                y_recv.at[r - 1, k], (q, source * 2 + core),
            ).wait_recv()
            total = total + ybuf[source, blk, :, within(span)].astype(f32)

        @pl.when(k == 0)
        def _():
            sums[q, :, within(span)] = total.astype(bf16)

        @pl.when(k > 0)
        def _():
            part[mine_at] = total.astype(bf16)
            remote(
                part.at[mine_at], sums.at[q, :, within(span)], z_send, z_recv.at[k], (blk, t)
            ).start()

    def all_back(part, sums, z_recv, span):
        def one(k, carry):
            source = (q + n_ep - k) % n_ep
            remote(
                part.at[t, 0, :, within(span)], sums.at[source, :, within(span)], z_send,
                z_recv.at[k], (source, t),
            ).wait_recv()
            return carry

        lax.fori_loop(1, n_ep, one, 0)

    full = (0, width)
    cut = width // 128 * 2 // 3 * 128
    spans = ((0, cut), (cut, width - cut))
    rows_h = rows_gu.at[:, pl.ds(0, ff)]

    def down_phase(j, carry):
        yy = (y + 1 + j) % n_y
        product(part_d, yy * 2 + 1 - core, rows_h, wd_v, full)
        to_pair(part_d, pair_d, pair_recv_d, full, yy).start()
        product(part_d, yy * 2 + core, rows_h, wd_v, full)
        from_pair(part_d, pair_d, pair_recv_d, full, yy)

        @pl.when(j < n_y - 1)
        def _():
            def one(k, carry_k):
                over_y(part_d, pair_d, ybuf_d, y_recv_d, full, j + 1, k)
                return carry_k

            lax.fori_loop(0, n_ep, one, 0)

        return carry

    lax.fori_loop(0, n_y, down_phase, 0)
    last_pieces(gslot_ref, ups_sems)
    finish(gslot_ref, ups_sems)

    rest_rows = all_rows.at[pl.ds(0, count - 1)]
    pltpu.make_async_copy(rest_rows, rest_rows, rew_recv).wait()
    rewards = jnp.sum(all_rows[...], axis=0)[0:1] / math.sqrt(SEQ_LEN)
    seq_total = pair_ref.shape[1]
    rew_ref[...] = rewards[:, :seq_total]
    pairs = seq_total // 2
    pair_lane = lax.broadcasted_iota(jnp.int32, (pairs, lanes), 1).astype(f32)
    order_lane = lax.broadcasted_iota(jnp.int32, (pairs, seq_total), 1)
    order_pair = 2 * lax.broadcasted_iota(jnp.int32, (pairs, seq_total), 0)
    order = pair_ref[...].astype(f32)

    def members(which):
        taken = jnp.where(order_lane == order_pair + which, order, 0.0)
        return (pair_lane == jnp.sum(taken, axis=1, keepdims=True)).astype(f32)

    chosen, rejected = members(0), members(1)
    margin = jnp.sum((chosen - rejected) * rewards, axis=1, keepdims=True)
    losses = jnp.maximum(-margin, 0.0) + jnp.log1p(jnp.exp(-jnp.abs(margin)))
    loss_ref[...] = jnp.sum(losses, axis=0, keepdims=True) / pairs
    pair_weight = jax.nn.sigmoid(-margin)
    seq_coef = jnp.sum(pair_weight * (rejected - chosen), axis=0, keepdims=True)
    slot_coef = seq_scale * jnp.sum(
        jnp.where(meta[...] > 0.0, seq_coef, 0.0), axis=1, keepdims=True
    )
    coef_wide = jnp.broadcast_to(slot_coef, coef_col.shape)
    coef_col[...] = coef_wide
    coef_row[...] = coef_wide.T[0:8]

    pieces = 1
    groups = chunks // pieces
    gc = fc * pieces

    def group(c):
        return pl.ds(pl.multiple_of(c * gc, gc), gc)

    def back_some(c):
        for j in range(per):
            k = c * per + j
            over_z(part_d, pair_d, ybuf_d, sums_d, y_recv_d, z_recv_d, full, (k + 1) % n_ep)

    def upstream(c):
        return dot(wd_v[group(c), :], gslot_ref[...].reshape(rows, depth), NT)

    def gradients(c, columns_up):
        hidden_grad = share_row[0:1, :] * (
            columns_up + coef_row[0:1, :] * wide(hc[group(c), :])
        )
        gate_grad = (hidden_grad * act_a[group(c), :]).astype(bf16)
        up_grad = (hidden_grad * act_b[group(c), :]).astype(bf16)
        gg_ref[group(c), :] = gate_grad
        ug_ref[group(c), :] = up_grad
        keep(1, gg_ref, gg_hbm, group(c)).start()
        keep(2, ug_ref, ug_hbm, group(c)).start()
        gate_t = gate_grad.astype(f32).T.astype(bf16)
        up_t = up_grad.astype(f32).T.astype(bf16)
        for i in range(pieces):
            first_at = (c * pieces + i) * 2 * fc
            part_of = slice(i * fc, (i + 1) * fc)
            rows_gu[:, pl.ds(pl.multiple_of(first_at, fc), fc)] = gate_t[:, part_of]
            rows_gu[:, pl.ds(pl.multiple_of(first_at + fc, fc), fc)] = up_t[:, part_of]

    def gradient_phase(c, carry):
        back_some(c - 1)
        following = upstream(c)
        gradients(c - 1, carry)
        return following

    last_up = lax.fori_loop(1, groups, gradient_phase, upstream(0))
    back_some(groups - 1)
    gradients(groups - 1, last_up)

    both = wgu_v.reshape(2 * ff, depth)

    share_of = n_ep // n_tp

    def return_some(h, i):
        for j in range(share_of):
            k = i * share_of + j
            over_z(
                part_i, pair_i, ybuf_i, sums_i, y_recv_i.at[h], z_recv_i.at[h], spans[h],
                (k + 1) % n_ep,
            )

    def serve(h, i):
        if h == 1:
            return_some(0, i)

    for h in range(2):
        def input_phase(j, carry, h=h):
            yy = (y + 1 + j) % n_y
            product(part_i, yy * 2 + 1 - core, rows_gu, both, spans[h])
            to_pair(part_i, pair_i, pair_recv_i.at[h], spans[h], yy).start()
            serve(h, 2 * j)
            product(part_i, yy * 2 + core, rows_gu, both, spans[h])
            serve(h, 2 * j + 1)
            from_pair(part_i, pair_i, pair_recv_i.at[h], spans[h], yy)

            @pl.when(j < n_y - 1)
            def _():
                def one(k, carry_k):
                    over_y(part_i, pair_i, ybuf_i, y_recv_i.at[h], spans[h], j + 1, k)
                    return carry_k

                lax.fori_loop(0, n_ep, one, 0)

            return carry

        lax.fori_loop(0, n_y, input_phase, 0)

    drain(gslot_ref.at[:, :, pl.ds(0, (n_tp - 1) * width)], ups_tp_send)

    def tail_phase(k, carry):
        row_at = pl.ds(pl.multiple_of(k * cap, cap), cap)
        coef_k = coef_col[row_at, 0:1]
        share_k = jnp.sum(meta[row_at, :], axis=1, keepdims=True)
        for owner in range(n_tp):
            cols = pl.ds(owner * width, width)
            head_k = head_all[owner][0:1, :]
            slot_out = (gslot_ref[k, :, cols].astype(f32) + coef_k * head_k).astype(bf16)
            gslot_ref[k, :, cols] = (share_k * slot_out.astype(f32)).astype(bf16)
        over_z(
            part_i, pair_i, ybuf_i, sums_i, y_recv_i.at[1], z_recv_i.at[1], spans[1],
            (k + 1) % n_ep,
        )
        pltpu.make_async_copy(gslot_ref.at[k], gslot_hbm.at[k], big_sem.at[1]).start()
        return carry

    lax.fori_loop(0, n_ep, tail_phase, 0)

    all_back(part_d, sums_d, z_recv_d, full)
    rest = mixing[...]
    mixed = tok_ref[...].astype(f32)
    expert_sums = sums_d[...].reshape(rows, width)
    for _ in range(3):
        piece = rest.astype(bf16)
        mixed = mixed + dot(piece, expert_sums)
        rest = rest - piece.astype(f32)
    layer_ref[...] = mixed.astype(bf16)
    finals = [
        pltpu.make_async_copy(src, dst, small_sem.at[i])
        for i, (src, dst) in enumerate(
            (
                (layer_ref, layer_hbm), (rew_ref, rew_hbm),
                (loss_ref, loss_hbm), (gtok_ref, gtok_hbm),
            )
        )
    ]
    for copy in finals[:3]:
        copy.start()
    token_coef = jnp.sum(jnp.where(in_seq, seq_coef, 0.0), axis=1, keepdims=True)
    grad_out = (ups_ref[...].astype(f32) + seq_scale * token_coef * head_mine).astype(bf16)
    for h in range(2):
        all_back(part_i, sums_i, z_recv_i.at[h], spans[h])
    returned = dot(picks[...], sums_i[...].reshape(rows, width))
    gtok_ref[...] = (grad_out.astype(f32) + returned).astype(bf16)
    finals[3].start()

    for copy in finals:
        copy.wait()
    slots_out.wait()
    pltpu.make_async_copy(gslot_ref, gslot_hbm, big_sem.at[1]).wait()
    for i, (src, dst) in enumerate(((hid_ref, hid_hbm), (gg_ref, gg_hbm), (ug_ref, ug_hbm))):
        keep(i, src, dst, pl.ds(0, ff)).wait()
    drain(sums_d.at[pl.ds(0, n_ep - 1)], a2a_send)
    drain(sums_d.at[pl.ds(0, n_ep - 1)], a2a_send)
    drain(raw_all.at[pl.ds(0, n_ep - 1)], raw_send)
    drain(head_all.at[pl.ds(0, n_tp - 1)], head_send)
    drain(slots_ref.at[:, :, pl.ds(0, (n_tp - 1) * width)], tok_tp_send)
    drain(rest_rows, rew_send)
    for _ in range(2):
        drain(pair_d, pair_send)
        if n_y > 1:
            drain(ybuf_d.at[pl.ds(0, n_y - 1)], y_send)
        drain(sums_d.at[pl.ds(0, n_ep - 1)], z_send)


def run_layer(
    expert_ids, share, tokens, upstream, head, order, w_gate, w_up, w_down, cap
):
    n_ep = lax.axis_size("ep")
    n_tp = lax.axis_size("tp")
    n_y = n_tp // 2
    tok_count, width = tokens.shape
    ff, depth = w_gate.shape
    rows = n_ep * cap
    steps = math.gcd(ff // 256, n_ep)
    chunks = max(steps // 2, 1)
    fc = ff // chunks
    seq_total = order.shape[1]
    lanes = 128 * pl.cdiv(seq_total, 128)
    dma = pltpu.SemaphoreType.DMA
    vmem = pl.BlockSpec(memory_space=pltpu.VMEM)
    hbm = pl.BlockSpec(memory_space=pl.ANY)

    def shape(*dims, kind=bf16):
        return jax.ShapeDtypeStruct(dims, kind)

    def scratch(*dims, kind=bf16):
        return pltpu.VMEM(dims, kind)

    back = [
        scratch(n_tp, n_ep, cap, width), scratch(n_y, n_ep, cap, width),
        scratch(n_y, n_ep, cap, width), scratch(n_ep, cap, width),
    ]
    return pl.pallas_call(
        partial(layer_kernel, n_ep, n_tp, steps, chunks),
        out_shape=(
            shape(n_ep, cap, depth), shape(n_ep, cap, depth),
            shape(ff, rows), shape(ff, rows), shape(ff, rows),
            shape(tok_count, width), shape(tok_count, width),
            shape(1, seq_total, kind=f32), shape(1, 1, kind=f32),
        ),
        in_specs=[vmem] * 2 + [hbm] * 2 + [vmem] * 2 + [hbm] * 3,
        out_specs=[hbm] * 9,
        scratch_shapes=[
            scratch(n_ep, cap, depth), scratch(n_ep, cap, depth),
            scratch(ff, rows), scratch(ff, rows), scratch(ff, rows),
            scratch(tok_count, width), scratch(tok_count, width),
            scratch(8, tok_count, kind=f32), scratch(8, width, kind=f32),
            scratch(tok_count, width), scratch(tok_count, width),
            scratch(1, seq_total, kind=f32), scratch(1, 1, kind=f32),
            scratch(chunks, 2 * fc, depth), scratch(ff, depth),
            scratch(EXPERTS, cap, width), scratch(EXPERTS, cap, width),
            scratch(n_ep, 8, tok_count, kind=f32), scratch(n_tp, 8, width, kind=f32),
            scratch(16, depth), scratch(ff, 128, kind=f32),
            scratch(tok_count, rows, kind=f32), scratch(tok_count, rows),
            scratch(rows, lanes, kind=f32), scratch(lanes, rows, kind=f32),
            scratch(ff, rows, kind=f32), scratch(ff, rows, kind=f32),
            scratch(rows, 2 * ff),
            scratch(8, rows, kind=f32), scratch(8, lanes, kind=f32),
            scratch(n_ep * n_tp, 8, lanes, kind=f32),
            scratch(8, rows, kind=f32), scratch(8, rows, kind=f32), scratch(rows, 128, kind=f32),
        ] + back + back + [
            dma((2,)), dma((3,)), dma((2,)), dma((4,)),
            dma((3, steps)), dma((4,)), dma, dma((n_ep,)), dma((n_ep,)), dma, dma((n_ep,)),
            dma, dma((n_tp,)), dma, dma((n_tp - 1, n_ep)), dma, dma((n_tp - 1, n_ep)), dma, dma,
            dma, dma((n_y,)), dma((2, n_y)), dma, dma((n_y - 1, n_ep)), dma((2, n_y - 1, n_ep)),
            dma, dma((n_ep,)), dma((2, n_ep)),
        ],
        compiler_params=pltpu.CompilerParams(
            collective_id=0, has_side_effects=True, vmem_limit_bytes=67000000
        ),
        name="run_layer",
    )(expert_ids, share, tokens, upstream, head, order, w_gate, w_up, w_down)


def grads_kernel(
    hid_ref, gg_ref, ug_ref, slots_ref, gslot_ref, layer_in, gtok_in, rew_in, loss_in,
    down_ref, gate_ref, up_ref, layer_ref, gtok_ref, rew_ref, loss_ref,
):
    @pl.when(pl.program_id(0) == 0)
    def _():
        layer_ref[...] = layer_in[...]
        gtok_ref[...] = gtok_in[...]
        rew_ref[...] = rew_in[...]
        loss_ref[...] = loss_in[...]

    inputs = slots_ref[...]
    down_ref[...] = dot(hid_ref[...], gslot_ref[...]).astype(bf16)
    gate_ref[...] = dot(gg_ref[...], inputs).astype(bf16)
    up_ref[...] = dot(ug_ref[...], inputs).astype(bf16)


def weight_grads(hid, gg, ug, slots, gslots, *small):
    ff, rows = hid.shape
    depth = slots.shape[1]
    block = 512 if depth % 512 == 0 else 128

    def whole(array):
        return pl.BlockSpec(array.shape, lambda i: (0, 0))

    left = pl.BlockSpec((ff, rows), lambda i: (0, 0))
    right = pl.BlockSpec((rows, block), lambda i: (0, i))
    out = pl.BlockSpec((ff, block), lambda i: (0, i))
    return pl.pallas_call(
        grads_kernel,
        grid=(depth // block,),
        out_shape=(jax.ShapeDtypeStruct((ff, depth), bf16),) * 3
        + tuple(jax.ShapeDtypeStruct(array.shape, array.dtype) for array in small),
        in_specs=[left, left, left, right, right] + [whole(array) for array in small],
        out_specs=[out] * 3 + [whole(array) for array in small],
        compiler_params=pltpu.CompilerParams(vmem_limit_bytes=67000000),
        cost_estimate=pl.CostEstimate(
            flops=6 * ff * rows * depth, bytes_accessed=6 * ff * depth, transcendentals=0
        ),
        name="weight_grads",
    )(hid, gg, ug, slots, gslots, *small)


def per_device(
    tokens, expert_ids, route_share, w_gate, w_up, w_down, reward_head, upstream, pair_order
):
    tok_count = tokens.shape[0]
    cap = tok_count * expert_ids.shape[1] // EXPERTS
    slots, gslots, hid, gg, ug, *small = run_layer(
        expert_ids.T, route_share.reshape(1, -1), tokens, upstream, reward_head.reshape(-1, 128),
        pair_order.reshape(1, -1), w_gate, w_up, w_down, cap,
    )
    depth = slots.shape[2]
    grad_down, grad_gate, grad_up, layer_out, grad_tokens, rew, loss = weight_grads(
        hid, gg, ug, slots.reshape(-1, depth), gslots.reshape(-1, depth), *small
    )
    return (
        layer_out, rew.reshape(-1), loss.reshape(()), grad_tokens, grad_gate, grad_up, grad_down
    )


def solution(mesh):
    in_specs = (
        P("ep", "tp"),
        P("ep", None),
        P("ep"),
        P(("ep", "tp"), None),
        P(("ep", "tp"), None),
        P(("ep", "tp"), None),
        P("tp"),
        P("ep", "tp"),
        P(),
    )
    out_specs = (
        P("ep", "tp"),
        P(),
        P(),
        P("ep", "tp"),
        P(("ep", "tp"), None),
        P(("ep", "tp"), None),
        P(("ep", "tp"), None),
    )
    return jax.shard_map(
        per_device, mesh=mesh, in_specs=in_specs, out_specs=out_specs, check_vma=False
    )
```
